256 devices in a mesh: dp: 32 (over z_hi, y, core), node: 8 (over z_lo, x).
Axes of the slice: x: 4, y: 4, z: 8 (z_hi: 4, z_lo: 2; z = z_hi * 2 + z_lo), core: 2. Of those that a mesh axis runs over, the one named last changes fastest.
Arguments:
- node_feats: bfloat16 [6144, 25, 128], P(('dp', 'node')), may hold values from -2 to 2
- cotangent: bfloat16 [6144, 25, 128], P(('dp', 'node')), may hold values from -3 to 3
- wigner: bfloat16 [13, 25, 65536], P(None, None, ('dp', 'node')), may hold values from -1.25 to 1.25
- radial: bfloat16 [2, 65536, 128], P(None, ('dp', 'node')), may hold values from 0.29882812 to 3
- edge_src: int32 [65536], P(('dp', 'node')), may hold values from 0 to 23
- edge_dst: int32 [65536], P(('dp', 'node')), may hold values from 0 to 23
- edge_count: int32 [256], P(('dp', 'node')), may hold values from 128 to 256
- params: float32 [2, 933888], P(None, ('dp', 'node')), may hold values from -0.5 to 0.5
- moment1: float32 [2, 933888], P(None, ('dp', 'node')), may hold values from -3 to 3
- moment2: float32 [2, 933888], P(None, ('dp', 'node')), may hold values from 1 to 100
Outputs:
- new_params: float32 [2, 933888], P(None, ('dp', 'node'))
- new_moment1: float32 [2, 933888], P(None, ('dp', 'node'))
- new_moment2: float32 [2, 933888], P(None, ('dp', 'node'))
The draws below stay inside these ranges and needn't reach their ends.
Inputs may be any that keep to these rules, and one draw needn't show every extreme that they name: `edge_src`: atom numbers within the edge's own structure. `edge_dst`: atom numbers within the edge's own structure. `edge_count`: slots from this number on within a structure are padding.
All inputs are finite; a program needn't handle non-finite values.
Results may differ from the reference program's by a relative error of at most 0.017.
Values may be sent and summed in bfloat16 or wider, within the bound.
No kernel may reach another device: no remote copies, remote signals or barrier semaphores. Data moves between devices by JAX's collectives and lax.ppermute only.
A program may use at most 64 MiB of HBM per device.

```python
import math
import jax
import jax.numpy as jnp
from jax import lax

C = 128
LMAX = 4
LAYERS = 2
NAT = 24
E_DEV = 256
COEF = 25
ROWS = 13
AVG = 10
PARAMS_LAYER = 933888
ATOMS = 6144
EDGES = 65536
DEVICES = 256


def plant(result, key, low, top_value):
    longest = result.shape.index(max(result.shape))
    spots = []
    for shift in (0, 1):
        where = [jax.random.randint(jax.random.fold_in(key, axis), (), 0, length) for axis, length in enumerate(result.shape)]
        where[longest] = (where[longest] + shift) % result.shape[longest]
        spots.append(tuple(where))
    return result.at[spots[0]].set(low).at[spots[1]].set(top_value)


def block_scale(own_key, dims, shards, smallest, high):
    def one(position, blocks):
        steps = jax.random.uniform(jax.random.fold_in(jax.random.fold_in(own_key, 6), position), (blocks,), jnp.float32, smallest / len(shards), high / len(shards))
        return jnp.repeat(jnp.exp(steps), dims[position] // blocks).reshape((-1,) + (1,) * (len(dims) - position - 1))

    gain = one(*shards[0])
    for cut in shards[1:]:
        gain = gain * one(*cut)
    return gain


def scatter_about(own_key, dims, width, limit, cuts=(), kind=jnp.bfloat16):
    result = width * jax.random.normal(own_key, dims, jnp.float32)
    if cuts:
        result = result * block_scale(own_key, dims, cuts, -0.22, 0.18)
    return jnp.clip(result, -limit, limit).astype(kind)


def setup_inputs(seed: int = 0) -> dict:
    keys = jax.random.split(jax.random.key(seed), 11)
    node_feats = scatter_about(keys[0], (ATOMS, COEF, C), 0.25, 2.0, ((0, 256),))
    cotangent = scatter_about(keys[1], (ATOMS, COEF, C), 0.5, 3.0, ((0, 256),))
    wigner = scatter_about(keys[2], (ROWS, COEF, EDGES), COEF ** -0.5, 1.25, ((2, 256),))
    radial = jnp.clip(jnp.exp(math.log(3.0) - 2.306499 * jax.random.uniform(keys[3], (LAYERS, EDGES, C), jnp.float32) ** block_scale(keys[3], (LAYERS, EDGES, C), ((1, 256),), -0.2, 0.2)), 0.29882812, 3.0).astype(jnp.bfloat16)
    edge_src = plant(jax.random.randint(keys[4], (EDGES,), 0, NAT), jax.random.fold_in(keys[4], 1), 0, NAT - 1).astype(jnp.int32)
    edge_dst = plant(jax.random.randint(keys[5], (EDGES,), 0, NAT), jax.random.fold_in(keys[5], 1), 0, NAT - 1).astype(jnp.int32)
    edge_count = plant(jax.random.randint(keys[6], (DEVICES,), E_DEV // 2, E_DEV + 1), jax.random.fold_in(keys[6], 1), E_DEV // 2, E_DEV).astype(jnp.int32)
    params = scatter_about(keys[7], (LAYERS, PARAMS_LAYER), ((LMAX + 1) * C // 4) ** -0.5, 0.5, ((1, 256),), jnp.float32)
    moment1 = scatter_about(keys[8], (LAYERS, PARAMS_LAYER), 0.5, 3.0, ((1, 256),), jnp.float32)
    moment2 = jnp.clip(jnp.exp(math.log(100.0) - 4.6051702 * jax.random.uniform(keys[9], (LAYERS, PARAMS_LAYER), jnp.float32) ** block_scale(keys[9], (LAYERS, PARAMS_LAYER), ((1, 256),), -0.2, 0.2)), 1.0, 100.0)
    return dict(node_feats=node_feats, cotangent=cotangent, wigner=wigner, radial=radial, edge_src=edge_src, edge_dst=edge_dst, edge_count=edge_count, params=params, moment1=moment1, moment2=moment2)


def layer(x, flat, wig, rad, src, dst, valid):
    nat, coef, chan = x.shape
    rows = wig.shape[0]
    lone = (rows + 2) // 3
    lmore = lone - 1
    edges = src.shape[0]
    kzero = lone * chan
    kone = lmore * chan
    xs = jnp.take(x, src, axis=0)
    rot = jnp.einsum('kje,ejc->ekc', wig.astype(jnp.float32), xs.astype(jnp.float32))
    rot = (rot * rad.astype(jnp.float32)[:, None, :]).astype(jnp.bfloat16)
    azero = rot[:, :lone].reshape(edges, kzero)
    aplus = rot[:, lone:lone + lmore].reshape(edges, kone)
    aminus = rot[:, lone + lmore:].reshape(edges, kone)
    wzero = flat[:kzero * kzero].reshape(kzero, kzero)
    wreal = flat[kzero * kzero:kzero * kzero + kone * kone].reshape(kone, kone)
    wimag = flat[kzero * kzero + kone * kone:].reshape(kone, kone)
    yzero = jnp.dot(azero, wzero, preferred_element_type=jnp.float32)
    yplus = jnp.dot(aplus, wreal, preferred_element_type=jnp.float32) - jnp.dot(aminus, wimag, preferred_element_type=jnp.float32)
    yminus = jnp.dot(aplus, wimag, preferred_element_type=jnp.float32) + jnp.dot(aminus, wreal, preferred_element_type=jnp.float32)
    mixed = jnp.concatenate([yzero.reshape(edges, lone, chan), yplus.reshape(edges, lmore, chan), yminus.reshape(edges, lmore, chan)], axis=1).astype(jnp.bfloat16)
    message = jnp.einsum('kje,ekc->ejc', wig.astype(jnp.float32), mixed.astype(jnp.float32)) * valid[:, None, None]
    aggregated = jax.ops.segment_sum(message, dst, num_segments=nat) / AVG
    out = x.astype(jnp.float32) + aggregated
    scalar = out[:, 0, :]
    gated = jnp.concatenate([jax.nn.silu(scalar)[:, None, :], out[:, 1:, :] * jax.nn.sigmoid(scalar)[:, None, :]], axis=1)
    return gated.astype(jnp.bfloat16)

def reference(node_feats, cotangent, wigner, radial, edge_src, edge_dst, edge_count, params, moment1, moment2):
    weights = params.astype(jnp.bfloat16)
    feats = node_feats.reshape(DEVICES, NAT, COEF, C)
    cots = cotangent.reshape(DEVICES, NAT, COEF, C)
    wigs = jnp.moveaxis(wigner.reshape(ROWS, COEF, DEVICES, E_DEV), 2, 0)
    rads = jnp.moveaxis(radial.reshape(LAYERS, DEVICES, E_DEV, C), 1, 0)
    sources = edge_src.reshape(DEVICES, E_DEV)
    targets = edge_dst.reshape(DEVICES, E_DEV)

    def structure(carry, item):
        feat, cot, wig, rad, src, dst, count = item
        valid = (jnp.arange(E_DEV, dtype=jnp.int32) < count).astype(jnp.float32)

        def forward(wts):
            hidden = layer(feat, wts[0], wig, rad[0], src, dst, valid)
            return layer(hidden, wts[1], wig, rad[1], src, dst, valid)
        _, pull = jax.vjp(forward, weights)
        grad_dev, = pull(cot)
        return (carry + grad_dev.astype(jnp.float32), None)
    start = jnp.zeros((LAYERS, PARAMS_LAYER), jnp.float32)
    grad, _ = lax.scan(structure, start, (feats, cots, wigs, rads, sources, targets, edge_count))
    new_moment1 = 0.9 * moment1 + 0.1 * grad
    new_moment2 = 0.95 * moment2 + 0.05 * grad * grad
    m_hat = new_moment1 / (1.0 - 0.9 ** 60)
    v_hat = new_moment2 / (1.0 - 0.95 ** 60)
    new_params = params - 0.01 * (m_hat / (jnp.sqrt(v_hat) + 1e-08) + 0.1 * params)
    return (new_params, new_moment1, new_moment2)
```

```python
import functools

import jax
import jax.numpy as jnp
from jax import lax
from jax.experimental import pallas as pl
from jax.experimental.pallas import tpu as pltpu
from jax.sharding import Mesh
from jax.sharding import PartitionSpec as P

F32 = jnp.float32
BF16 = jnp.bfloat16
AVG = 10
AXES = ("zh", "y", "core", "zl", "x")
SIZES = (4, 4, 2, 2, 4)
NEAR = ("y", "zl")
FAR = ("zh", "x")
LANES = 128


def mm(a, b):
    return lax.dot_general(a, b, (((1,), (0,)), ((), ())), preferred_element_type=F32)


def mm_bt(a, b):
    return lax.dot_general(a, b, (((1,), (1,)), ((), ())), preferred_element_type=F32)


def mm_at(a, b):
    return lax.dot_general(a, b, (((0,), (0,)), ((), ())), preferred_element_type=F32)


def prep_kernel(nat, wig_ref, src_ref, dst_ref, srcc_ref, dstc_ref, x_ref, rad_ref, a_ref, b_ref, bt_ref, d_ref, dt_ref):
    rows, coef, edges = wig_ref.shape
    wide = coef * nat
    chan = x_ref.shape[1]
    lane = lax.broadcasted_iota(jnp.int32, (coef, wide), 1)
    start = lax.broadcasted_iota(jnp.int32, (coef, wide), 0) * nat
    spread = ((lane >= start) & (lane < start + nat)).astype(BF16)
    lane_e = lax.broadcasted_iota(jnp.int32, (edges, wide), 1) % nat
    row_e = lax.broadcasted_iota(jnp.int32, (wide, edges), 0) % nat
    pick_src = (lane_e == srcc_ref[...]).astype(F32).astype(BF16)
    pick_dst = (lane_e == dstc_ref[...]).astype(F32).astype(BF16)
    pick_src_t = (row_e == src_ref[...]).astype(F32).astype(BF16)
    pick_dst_t = (row_e == dst_ref[...]).astype(F32).astype(BF16)
    x = x_ref[...]
    rad = rad_ref[...].astype(F32)
    for k in range(rows):
        w = wig_ref[k]
        e_wide = mm_at(w, spread).astype(BF16)
        wide_e = mm_at(spread, w).astype(BF16)
        b = e_wide * pick_src
        b_ref[k] = b
        d_ref[k] = e_wide * pick_dst
        bt_ref[k] = wide_e * pick_src_t
        dt_ref[k] = wide_e * pick_dst_t
        a_ref[:, k * chan : (k + 1) * chan] = (mm(b, x) * rad).astype(BF16)


def rotate(b_ref, x, rad, a_ref):
    chan = x.shape[1]
    for k in range(b_ref.shape[0]):
        a_ref[:, k * chan : (k + 1) * chan] = (mm(b_ref[k], x) * rad).astype(BF16)


def mix(a_ref, w0, wr, wi, m_ref):
    kz, ko = w0.shape[0], wr.shape[0]
    m_ref[:, :kz] = mm(a_ref[:, :kz], w0[...]).astype(BF16)
    ap = a_ref[:, kz : kz + ko]
    am = a_ref[:, kz + ko :]
    m_ref[:, kz : kz + ko] = (mm(ap, wr[...]) - mm(am, wi[...])).astype(BF16)
    m_ref[:, kz + ko :] = (mm(ap, wi[...]) + mm(am, wr[...])).astype(BF16)


def back_to_nodes(t_ref, m_ref, chan):
    total = mm(t_ref[0], m_ref[:, :chan])
    for k in range(1, t_ref.shape[0]):
        total = total + mm(t_ref[k], m_ref[:, k * chan : (k + 1) * chan])
    return total


def gate(out, nat):
    o = out.reshape(-1, nat, out.shape[1])
    s = o[0]
    sig = jax.nn.sigmoid(s)
    h = jnp.concatenate([(s * sig)[None], o[1:] * sig[None]], axis=0)
    return h.reshape(out.shape)


def gate_back(dh, out, nat):
    o = out.reshape(-1, nat, out.shape[1])
    g = dh.reshape(o.shape)
    s = o[0]
    sig = jax.nn.sigmoid(s)
    slope = sig * (1.0 - sig)
    down = jnp.sum(g[1:] * o[1:], axis=0) * slope + g[0] * (sig + s * slope)
    d = jnp.concatenate([down[None], g[1:] * sig[None]], axis=0)
    return d.reshape(out.shape)


def pieces(kz, ko):
    first = kz * (kz // LANES)
    second = first + ko * (ko // LANES)
    return ((0, kz, kz // LANES), (first, ko, ko // LANES), (second, ko, ko // LANES))


def chunk_at(g, core, zh):
    y, zl = divmod(g, 2)
    return ((zh * 4 + y) * 2 + core) * 2 + zl


def unpack(core, mine, other, flat, stage, weights):
    groups, rows, _ = mine.shape
    part = rows // 4
    for g in range(groups):
        m = mine[g].astype(F32)
        o = other[g].astype(F32)
        for c in range(2):
            stage[c] = jnp.where(core == c, m, o)
            for zh in range(4):
                at = chunk_at(g, c, zh) * part
                flat[at : at + part] = stage[c, zh * part : (zh + 1) * part]
    for ref, (first, side, step) in zip(weights, pieces(weights[0].shape[0], weights[1].shape[0])):
        for q in range(step):
            ref[:, q * LANES : (q + 1) * LANES] = flat[pl.ds(first + q, side, stride=step), :].astype(BF16)


def pack(core, a_ref, dy_ref, kz, ko, flat, stage, keep, send):
    def put(grad, piece):
        first, side, step = piece
        for q in range(step):
            flat[pl.ds(first + q, side, stride=step), :] = grad[:, q * LANES : (q + 1) * LANES]

    p0, pr, pi = pieces(kz, ko)
    put(mm_at(a_ref[:, :kz], dy_ref[:, :kz]), p0)
    ap = a_ref[:, kz : kz + ko]
    am = a_ref[:, kz + ko :]
    dp = dy_ref[:, kz : kz + ko]
    dm = dy_ref[:, kz + ko :]
    put(mm_at(ap, dp) + mm_at(am, dm), pr)
    put(mm_at(ap, dm) - mm_at(am, dp), pi)
    groups, rows, _ = keep.shape
    part = rows // 4
    for g in range(groups):
        for c in range(2):
            for zh in range(4):
                at = chunk_at(g, c, zh) * part
                stage[c, zh * part : (zh + 1) * part] = flat[at : at + part]
        v0, v1 = stage[0], stage[1]
        keep[g] = jnp.where(core == 0, v0, v1).astype(BF16)
        send[g] = jnp.where(core == 0, v1, v0).astype(BF16)


def first_kernel(nat, core_ref, mine, other, a_ref, x_ref, dt_ref, out_ref, h_ref, flat, stage, w0, wr, wi, m_ref):
    unpack(core_ref[0], mine, other, flat, stage, (w0, wr, wi))
    mix(a_ref, w0, wr, wi, m_ref)
    out = x_ref[...].astype(F32) + back_to_nodes(dt_ref, m_ref, x_ref.shape[1]) / AVG
    out_ref[...] = out
    h_ref[...] = gate(out, nat).astype(BF16)


def middle_kernel(nat, core_ref, mine, other, out_ref, h_ref, cot_ref, rad_ref, b_ref, bt_ref, d_ref, dt_ref,
                  keep, send, dy0_ref, flat, stage, w0, wr, wi, a_ref, m_ref, dy_ref):
    chan = h_ref.shape[1]
    rows = b_ref.shape[0]
    kz, ko = w0.shape[0], wr.shape[0]
    rad = rad_ref[...].astype(F32)
    h1 = h_ref[...]
    rotate(b_ref, h1, rad, a_ref)
    unpack(core_ref[0], mine, other, flat, stage, (w0, wr, wi))
    mix(a_ref, w0, wr, wi, m_ref)
    out2 = h1.astype(F32) + back_to_nodes(dt_ref, m_ref, chan) / AVG
    dout2 = gate_back(cot_ref[...].astype(F32), out2, nat)
    dagg = (dout2 / AVG).astype(BF16)
    for k in range(rows):
        dy_ref[:, k * chan : (k + 1) * chan] = mm(d_ref[k], dagg).astype(BF16)
    pack(core_ref[0], a_ref, dy_ref, kz, ko, flat, stage, keep, send)
    dp = dy_ref[:, kz : kz + ko]
    dm = dy_ref[:, kz + ko :]
    parts = (
        mm_bt(dy_ref[:, :kz], w0[...]),
        mm_bt(dp, wr[...]) + mm_bt(dm, wi[...]),
        mm_bt(dm, wr[...]) - mm_bt(dp, wi[...]),
    )
    at = 0
    for part in parts:
        for q in range(part.shape[1] // chan):
            piece = part[:, q * chan : (q + 1) * chan].astype(BF16).astype(F32)
            m_ref[:, at : at + chan] = (piece * rad).astype(BF16)
            at += chan
    dh1 = (dout2 + back_to_nodes(bt_ref, m_ref, chan)).astype(BF16).astype(F32)
    dagg1 = (gate_back(dh1, out_ref[...], nat) / AVG).astype(BF16)
    for k in range(rows):
        dy0_ref[:, k * chan : (k + 1) * chan] = mm(d_ref[k], dagg1).astype(BF16)


def last_kernel(kz, ko, core_ref, a_ref, dy_ref, keep, send, flat, stage):
    pack(core_ref[0], a_ref, dy_ref, kz, ko, flat, stage, keep, send)


def sds(shape, dtype):
    return jax.ShapeDtypeStruct(shape, dtype)


def call(kernel, outs, args, scratch=(), scalars=0, flops=1 << 32, vmem=28 << 20):
    specs = [pl.BlockSpec(memory_space=pltpu.SMEM)] * scalars
    specs += [pl.BlockSpec(memory_space=pltpu.VMEM)] * (len(args) - scalars)
    return pl.pallas_call(
        kernel,
        out_shape=outs,
        in_specs=specs,
        out_specs=[pl.BlockSpec(memory_space=pltpu.VMEM)] * len(outs),
        scratch_shapes=scratch,
        compiler_params=pltpu.CompilerParams(vmem_limit_bytes=vmem),
        cost_estimate=pl.CostEstimate(flops=flops, bytes_accessed=1 << 20, transcendentals=0),
    )(*args)


def count_of(axes):
    n = 1
    for a in axes:
        n *= lax.axis_size(a)
    return n


def from_everyone(x, axes):
    spread = jnp.broadcast_to(x[None], (count_of(axes), *x.shape))
    return lax.all_to_all(spread, axes, 0, 0, tiled=True)


def swap_core(x):
    return lax.ppermute(x, "core", [(0, 1), (1, 0)])


def local(node_feats, cotangent, wigner, radial, edge_src, edge_dst, edge_count, params, moment1, moment2):
    nat, coef, chan = node_feats.shape
    rows, _, edges = wigner.shape
    lone = (rows + 2) // 3
    kz, ko = lone * chan, (lone - 1) * chan
    layers, shard = params.shape
    far, near = count_of(FAR), count_of(NEAR)
    core = lax.axis_index("core").astype(jnp.int32).reshape(1)
    block = far * shard // LANES

    got = from_everyone(params.astype(BF16), FAR)
    got = jnp.moveaxis(got, 1, 0).reshape(layers, block, LANES)
    mine = [from_everyone(got[i], NEAR) for i in range(layers)]
    other = [swap_core(m) for m in mine]

    x = jnp.transpose(node_feats, (1, 0, 2)).reshape(coef * nat, chan)
    cot = jnp.transpose(cotangent, (1, 0, 2)).reshape(coef * nat, chan)
    live = jnp.arange(edges, dtype=jnp.int32) < edge_count[0]
    dst = jnp.where(live, edge_dst, -1)
    wide = coef * nat
    mats = [sds((rows, edges, wide), BF16), sds((rows, wide, edges), BF16)] * 2
    act = sds((edges, rows * chan), BF16)
    a0, b, bt, d, dt = call(
        functools.partial(prep_kernel, nat),
        [act, *mats],
        (wigner, edge_src.reshape(1, edges), dst.reshape(1, edges), edge_src.reshape(edges, 1), dst.reshape(edges, 1), x, radial[0]),
        vmem=40 << 20,
    )
    flat = [pltpu.VMEM((kz * kz // LANES + 2 * ko * ko // LANES, LANES), F32), pltpu.VMEM((2, block, LANES), F32)]
    weights = [pltpu.VMEM((kz, kz), BF16), pltpu.VMEM((ko, ko), BF16), pltpu.VMEM((ko, ko), BF16)]
    space = pltpu.VMEM((edges, rows * chan), BF16)
    out1, h1 = call(
        functools.partial(first_kernel, nat),
        [sds((wide, chan), F32), sds((wide, chan), BF16)],
        (core, mine[0], other[0], a0, x, dt),
        [*flat, *weights, space],
        scalars=1,
    )
    halves = [sds((near, block, LANES), BF16)] * 2
    keep1, send1, dy0 = call(
        functools.partial(middle_kernel, nat),
        [*halves, act],
        (core, mine[1], other[1], out1, h1, cot, radial[1], b, bt, d, dt),
        [*flat, *weights, space, space, space],
        scalars=1,
        vmem=48 << 20,
    )
    keep0, send0 = call(
        functools.partial(last_kernel, kz, ko), halves, (core, a0, dy0), flat, scalars=1
    )

    def reduce_near(keep, send):
        pair = (keep.astype(F32) + swap_core(send).astype(F32)).astype(BF16)
        arrived = lax.all_to_all(pair, NEAR, 0, 0, tiled=True)
        return arrived.astype(F32).sum(axis=0)

    near1 = reduce_near(keep1, send1)
    near0 = reduce_near(keep0, send0)
    both = jnp.stack([near0, near1]).reshape(layers, far, shard)
    arrived = lax.all_to_all(jnp.moveaxis(both, 0, 1), FAR, 0, 0, tiled=True)
    grad = arrived.sum(axis=0)

    new_moment1 = 0.9 * moment1 + 0.1 * grad
    new_moment2 = 0.95 * moment2 + 0.05 * grad * grad
    m_hat = new_moment1 / (1.0 - 0.9**60)
    v_hat = new_moment2 / (1.0 - 0.95**60)
    new_params = params - 0.01 * (m_hat / (jnp.sqrt(v_hat) + 1e-08) + 0.1 * params)
    return (new_params, new_moment1, new_moment2)


def solution(mesh):
    fine = Mesh(mesh.devices.reshape(SIZES), AXES)
    flat = P(None, AXES)
    return jax.shard_map(
        local,
        mesh=fine,
        in_specs=(
            P(AXES, None, None),
            P(AXES, None, None),
            P(None, None, AXES),
            P(None, AXES, None),
            P(AXES),
            P(AXES),
            P(AXES),
            flat,
            flat,
            flat,
        ),
        out_specs=(flat, flat, flat),
        check_vma=False,
    )
```

```python
import functools

import jax
import jax.numpy as jnp
from jax import lax
from jax.experimental import pallas as pl
from jax.experimental.pallas import tpu as pltpu
from jax.sharding import Mesh
from jax.sharding import PartitionSpec as P

F32 = jnp.float32
BF16 = jnp.bfloat16
AVG = 10
AXES = ("zh", "y", "core", "zl", "x")
SIZES = (4, 4, 2, 2, 4)
NEAR = ("y", "zl", "x")
FAR = ("zh",)
LANES = 128


def mm(a, b):
    return lax.dot_general(a, b, (((1,), (0,)), ((), ())), preferred_element_type=F32)


def mm_bt(a, b):
    return lax.dot_general(a, b, (((1,), (1,)), ((), ())), preferred_element_type=F32)


def mm_at(a, b):
    return lax.dot_general(a, b, (((0,), (0,)), ((), ())), preferred_element_type=F32)


def prep_kernel(nat, wig_ref, src_ref, dst_ref, srcc_ref, dstc_ref, x_ref, rad_ref, a_ref, b_ref, bt_ref, d_ref, dt_ref):
    rows, coef, edges = wig_ref.shape
    wide = coef * nat
    chan = x_ref.shape[1]
    lane = lax.broadcasted_iota(jnp.int32, (coef, wide), 1)
    start = lax.broadcasted_iota(jnp.int32, (coef, wide), 0) * nat
    spread = ((lane >= start) & (lane < start + nat)).astype(BF16)
    lane_e = lax.broadcasted_iota(jnp.int32, (edges, wide), 1) % nat
    row_e = lax.broadcasted_iota(jnp.int32, (wide, edges), 0) % nat
    pick_src = (lane_e == srcc_ref[...]).astype(F32).astype(BF16)
    pick_dst = (lane_e == dstc_ref[...]).astype(F32).astype(BF16)
    pick_src_t = (row_e == src_ref[...]).astype(F32).astype(BF16)
    pick_dst_t = (row_e == dst_ref[...]).astype(F32).astype(BF16)
    x = x_ref[...]
    rad = rad_ref[...].astype(F32)
    for k in range(rows):
        w = wig_ref[k]
        e_wide = mm_at(w, spread).astype(BF16)
        wide_e = mm_at(spread, w).astype(BF16)
        b = e_wide * pick_src
        b_ref[k] = b
        d_ref[k] = e_wide * pick_dst
        bt_ref[k] = wide_e * pick_src_t
        dt_ref[k] = wide_e * pick_dst_t
        a_ref[:, k * chan : (k + 1) * chan] = (mm(b, x) * rad).astype(BF16)


def rotate(b_ref, x, rad, a_ref):
    chan = x.shape[1]
    for k in range(b_ref.shape[0]):
        a_ref[:, k * chan : (k + 1) * chan] = (mm(b_ref[k], x) * rad).astype(BF16)


def mix(a_ref, w0, wr, wi, m_ref):
    kz, ko = w0.shape[0], wr.shape[0]
    m_ref[:, :kz] = mm(a_ref[:, :kz], w0[...]).astype(BF16)
    ap = a_ref[:, kz : kz + ko]
    am = a_ref[:, kz + ko :]
    m_ref[:, kz : kz + ko] = (mm(ap, wr[...]) - mm(am, wi[...])).astype(BF16)
    m_ref[:, kz + ko :] = (mm(ap, wi[...]) + mm(am, wr[...])).astype(BF16)


def back_to_nodes(t_ref, m_ref, chan):
    total = mm(t_ref[0], m_ref[:, :chan])
    for k in range(1, t_ref.shape[0]):
        total = total + mm(t_ref[k], m_ref[:, k * chan : (k + 1) * chan])
    return total


def gate(out, nat):
    o = out.reshape(-1, nat, out.shape[1])
    s = o[0]
    sig = jax.nn.sigmoid(s)
    h = jnp.concatenate([(s * sig)[None], o[1:] * sig[None]], axis=0)
    return h.reshape(out.shape)


def gate_back(dh, out, nat):
    o = out.reshape(-1, nat, out.shape[1])
    g = dh.reshape(o.shape)
    s = o[0]
    sig = jax.nn.sigmoid(s)
    slope = sig * (1.0 - sig)
    down = jnp.sum(g[1:] * o[1:], axis=0) * slope + g[0] * (sig + s * slope)
    d = jnp.concatenate([down[None], g[1:] * sig[None]], axis=0)
    return d.reshape(out.shape)


def pieces(kz, ko):
    first = kz * (kz // LANES)
    second = first + ko * (ko // LANES)
    return ((0, kz, kz // LANES), (first, ko, ko // LANES), (second, ko, ko // LANES))


def chunks(core):
    zhs, ys, cores, zls, xs = SIZES
    for y in range(ys):
        for zl in range(zls):
            for x in range(xs):
                for zh in range(zhs):
                    owner = (((zh * ys + y) * cores + core) * zls + zl) * xs + x
                    yield owner // 2, owner % 2, (y * zls + zl) * xs + x, zh


def unpack(core, mine, other, flat, stage):
    layers = flat.shape[0]
    part = stage.shape[1] // (SIZES[0] * layers)
    pair = 2 * part - 1
    where = [list(chunks(c)) for c in range(2)]
    first = lax.broadcasted_iota(jnp.int32, (part, LANES), 0) == 0
    for g in range(mine.shape[0]):
        m = mine[g].astype(F32)
        o = other[g].astype(F32)
        for c in range(2):
            stage[c] = jnp.where(core == c, m, o)
            for row, odd, sender, zh in where[c]:
                if sender != g:
                    continue
                for i in range(layers):
                    at = (zh * layers + i) * part
                    block = stage[c, at : at + part]
                    to = row * pair + odd * (part - 1)
                    if odd:
                        block = jnp.where(first, block + flat[i, to : to + part], block)
                    flat[i, to : to + part] = block


def take_weights(flat, layer, weights):
    for ref, (first, side, step) in zip(weights, pieces(weights[0].shape[0], weights[1].shape[0])):
        for q in range(step):
            ref[:, q * LANES : (q + 1) * LANES] = flat[layer, pl.ds(first + q, side, stride=step), :].astype(BF16)


def put_grads(a_ref, dy_ref, kz, ko, layer, flat):
    def put(grad, piece):
        first, side, step = piece
        for q in range(step):
            flat[layer, pl.ds(first + q, side, stride=step), :] = grad[:, q * LANES : (q + 1) * LANES]

    p0, pr, pi = pieces(kz, ko)
    put(mm_at(a_ref[:, :kz], dy_ref[:, :kz]), p0)
    ap = a_ref[:, kz : kz + ko]
    am = a_ref[:, kz + ko :]
    dp = dy_ref[:, kz : kz + ko]
    dm = dy_ref[:, kz + ko :]
    put(mm_at(ap, dp) + mm_at(am, dm), pr)
    put(mm_at(ap, dm) - mm_at(am, dp), pi)


def pack(core, flat, stage, keep, send):
    layers = flat.shape[0]
    part = stage.shape[1] // (SIZES[0] * layers)
    pair = 2 * part - 1
    where = [list(chunks(c)) for c in range(2)]
    for g in range(keep.shape[0]):
        for c in range(2):
            for row, odd, sender, zh in where[c]:
                if sender != g:
                    continue
                for i in range(layers):
                    at = (zh * layers + i) * part
                    to = row * pair + odd * (part - 1)
                    stage[c, at : at + part] = flat[i, to : to + part]
        v0, v1 = stage[0], stage[1]
        keep[g] = jnp.where(core == 0, v0, v1).astype(BF16)
        send[g] = jnp.where(core == 0, v1, v0).astype(BF16)


def main_kernel(nat, core_ref, mine, other, a0_ref, x_ref, cot_ref, rad_ref, b_far, bt_far, d_far, dt_far,
                keep, send, flat, stage, w0, wr, wi, a_ref, m_ref, dy_ref, b_ref, bt_ref, d_ref, dt_ref, sems):
    moves = [
        pltpu.make_async_copy(far, near, sems.at[i])
        for i, (far, near) in enumerate(((dt_far, dt_ref), (b_far, b_ref), (d_far, d_ref), (bt_far, bt_ref)))
    ]
    for move in moves:
        move.start()
    chan = x_ref.shape[1]
    rows = b_ref.shape[0]
    kz, ko = w0.shape[0], wr.shape[0]
    core = core_ref[0]
    rad = rad_ref[...].astype(F32)
    unpack(core, mine, other, flat, stage)
    take_weights(flat, 0, (w0, wr, wi))
    mix(a0_ref, w0, wr, wi, m_ref)
    moves[0].wait()
    out1 = x_ref[...].astype(F32) + back_to_nodes(dt_ref, m_ref, chan) / AVG
    h1 = gate(out1, nat).astype(BF16)
    moves[1].wait()
    rotate(b_ref, h1, rad, a_ref)
    take_weights(flat, 1, (w0, wr, wi))
    mix(a_ref, w0, wr, wi, m_ref)
    out2 = h1.astype(F32) + back_to_nodes(dt_ref, m_ref, chan) / AVG
    dout2 = gate_back(cot_ref[...].astype(F32), out2, nat)
    dagg = (dout2 / AVG).astype(BF16)
    moves[2].wait()
    for k in range(rows):
        dy_ref[:, k * chan : (k + 1) * chan] = mm(d_ref[k], dagg).astype(BF16)
    put_grads(a_ref, dy_ref, kz, ko, 1, flat)
    dp = dy_ref[:, kz : kz + ko]
    dm = dy_ref[:, kz + ko :]
    parts = (
        mm_bt(dy_ref[:, :kz], w0[...]),
        mm_bt(dp, wr[...]) + mm_bt(dm, wi[...]),
        mm_bt(dm, wr[...]) - mm_bt(dp, wi[...]),
    )
    at = 0
    for part in parts:
        for q in range(part.shape[1] // chan):
            piece = part[:, q * chan : (q + 1) * chan].astype(BF16).astype(F32)
            m_ref[:, at : at + chan] = (piece * rad).astype(BF16)
            at += chan
    moves[3].wait()
    dh1 = (dout2 + back_to_nodes(bt_ref, m_ref, chan)).astype(BF16).astype(F32)
    dagg1 = (gate_back(dh1, out1, nat) / AVG).astype(BF16)
    for k in range(rows):
        dy_ref[:, k * chan : (k + 1) * chan] = mm(d_ref[k], dagg1).astype(BF16)
    put_grads(a0_ref, dy_ref, kz, ko, 0, flat)
    pack(core, flat, stage, keep, send)


def sds(shape, dtype):
    return jax.ShapeDtypeStruct(shape, dtype)


def call(kernel, outs, args, scratch=(), scalars=0, far=0, flops=1 << 32, vmem=28 << 20):
    specs = [pl.BlockSpec(memory_space=pltpu.SMEM)] * scalars
    specs += [pl.BlockSpec(memory_space=pltpu.VMEM)] * (len(args) - scalars - far)
    specs += [pl.BlockSpec(memory_space=pl.ANY)] * far
    return pl.pallas_call(
        kernel,
        out_shape=outs,
        in_specs=specs,
        out_specs=[pl.BlockSpec(memory_space=pltpu.VMEM)] * len(outs),
        scratch_shapes=scratch,
        compiler_params=pltpu.CompilerParams(vmem_limit_bytes=vmem),
        cost_estimate=pl.CostEstimate(flops=flops, bytes_accessed=1 << 20, transcendentals=0),
    )(*args)


def count_of(axes):
    n = 1
    for a in axes:
        n *= lax.axis_size(a)
    return n


def from_everyone(x, axes):
    spread = jnp.broadcast_to(x[None], (count_of(axes), *x.shape))
    return lax.all_to_all(spread, axes, 0, 0, tiled=True)


def swap_core(x):
    return lax.ppermute(x, "core", [(0, 1), (1, 0)])


def local(node_feats, cotangent, wigner, radial, edge_src, edge_dst, edge_count, params, moment1, moment2):
    nat, coef, chan = node_feats.shape
    rows, _, edges = wigner.shape
    lone = (rows + 2) // 3
    kz, ko = lone * chan, (lone - 1) * chan
    layers, shard = params.shape
    far, near = count_of(FAR), count_of(NEAR)
    core = lax.axis_index("core").astype(jnp.int32).reshape(1)
    odd = lax.axis_index("x") % 2 == 1
    part = (shard + LANES // 2) // LANES
    spare = part * LANES - shard

    half = params.astype(BF16)
    half = jnp.where(odd, jnp.pad(half, ((0, 0), (spare, 0))), jnp.pad(half, ((0, 0), (0, spare))))
    got = from_everyone(half.reshape(layers * part, LANES), FAR).reshape(far * layers * part, LANES)
    mine = from_everyone(got, NEAR)
    other = swap_core(mine)

    x = jnp.transpose(node_feats, (1, 0, 2)).reshape(coef * nat, chan)
    cot = jnp.transpose(cotangent, (1, 0, 2)).reshape(coef * nat, chan)
    live = jnp.arange(edges, dtype=jnp.int32) < edge_count[0]
    dst = jnp.where(live, edge_dst, -1)
    wide = coef * nat
    mats = [sds((rows, edges, wide), BF16), sds((rows, wide, edges), BF16)] * 2
    act = sds((edges, rows * chan), BF16)
    a0, b, bt, d, dt = call(
        functools.partial(prep_kernel, nat),
        [act, *mats],
        (wigner, edge_src.reshape(1, edges), dst.reshape(1, edges), edge_src.reshape(edges, 1), dst.reshape(edges, 1), x, radial[0]),
        vmem=24 << 20,
    )
    block = far * layers * part
    flat = [pltpu.VMEM((layers, (kz * kz + 2 * ko * ko) // LANES, LANES), F32), pltpu.VMEM((2, block, LANES), F32)]
    weights = [pltpu.VMEM((kz, kz), BF16), pltpu.VMEM((ko, ko), BF16), pltpu.VMEM((ko, ko), BF16)]
    space = pltpu.VMEM((edges, rows * chan), BF16)
    held = [pltpu.VMEM(m.shape, m.dtype) for m in mats]
    keep, send = call(
        functools.partial(main_kernel, nat),
        [sds((near, block, LANES), BF16)] * 2,
        (core, mine, other, a0, x, cot, radial[1], b, bt, d, dt),
        [*flat, *weights, space, space, space, *held, pltpu.SemaphoreType.DMA((len(held),))],
        scalars=1,
        far=len(held),
        vmem=44 << 20,
    )
    pair = (keep.astype(F32) + swap_core(send).astype(F32)).astype(BF16)
    arrived = lax.all_to_all(pair, NEAR, 0, 0, tiled=True)
    near_sum = arrived.astype(F32).sum(axis=0).reshape(far, layers * part, LANES)
    grad = lax.all_to_all(near_sum, FAR, 0, 0, tiled=True).sum(axis=0).reshape(layers, part * LANES)
    grad = jnp.where(odd, grad[:, spare:], grad[:, :shard])

    new_moment1 = 0.9 * moment1 + 0.1 * grad
    new_moment2 = 0.95 * moment2 + 0.05 * grad * grad
    m_hat = new_moment1 / (1.0 - 0.9**60)
    v_hat = new_moment2 / (1.0 - 0.95**60)
    new_params = params - 0.01 * (m_hat / (jnp.sqrt(v_hat) + 1e-08) + 0.1 * params)
    return (new_params, new_moment1, new_moment2)


def solution(mesh):
    fine = Mesh(mesh.devices.reshape(SIZES), AXES)
    flat = P(None, AXES)
    return jax.shard_map(
        local,
        mesh=fine,
        in_specs=(
            P(AXES, None, None),
            P(AXES, None, None),
            P(None, None, AXES),
            P(None, AXES, None),
            P(AXES),
            P(AXES),
            P(AXES),
            flat,
            flat,
            flat,
        ),
        out_specs=(flat, flat, flat),
        check_vma=False,
    )
```

```python
import functools

import jax
import jax.numpy as jnp
from jax import lax
from jax.experimental import pallas as pl
from jax.experimental.pallas import tpu as pltpu
from jax.sharding import Mesh
from jax.sharding import PartitionSpec as P

F32 = jnp.float32
BF16 = jnp.bfloat16
AVG = 10
AXES = ("zh", "y", "core", "zl", "x")
SIZES = (4, 4, 2, 2, 4)
NEAR = ("y", "zl", "x")
FAR = ("zh",)
LANES = 128
PAIRS = 128


def mm(a, b):
    return lax.dot_general(a, b, (((1,), (0,)), ((), ())), preferred_element_type=F32)


def mm_bt(a, b):
    return lax.dot_general(a, b, (((1,), (1,)), ((), ())), preferred_element_type=F32)


def mm_at(a, b):
    return lax.dot_general(a, b, (((0,), (0,)), ((), ())), preferred_element_type=F32)


def prep_kernel(nat, wig_ref, src_ref, dst_ref, srcc_ref, dstc_ref, x_ref, rad_ref, a_ref, b_ref, bt_ref, d_ref, dt_ref):
    rows, coef, edges = wig_ref.shape
    wide = coef * nat
    chan = x_ref.shape[1]
    lane = lax.broadcasted_iota(jnp.int32, (coef, wide), 1)
    start = lax.broadcasted_iota(jnp.int32, (coef, wide), 0) * nat
    spread = ((lane >= start) & (lane < start + nat)).astype(BF16)
    lane_e = lax.broadcasted_iota(jnp.int32, (edges, wide), 1) % nat
    row_e = lax.broadcasted_iota(jnp.int32, (wide, edges), 0) % nat
    pick_src = (lane_e == srcc_ref[...]).astype(F32).astype(BF16)
    pick_dst = (lane_e == dstc_ref[...]).astype(F32).astype(BF16)
    pick_src_t = (row_e == src_ref[...]).astype(F32).astype(BF16)
    pick_dst_t = (row_e == dst_ref[...]).astype(F32).astype(BF16)
    x = x_ref[...]
    rad = rad_ref[...].astype(F32)
    for k in range(rows):
        w = wig_ref[k]
        e_wide = mm_at(w, spread).astype(BF16)
        wide_e = mm_at(spread, w).astype(BF16)
        b = e_wide * pick_src
        b_ref[k] = b
        d_ref[k] = e_wide * pick_dst
        bt_ref[k] = wide_e * pick_src_t
        dt_ref[k] = wide_e * pick_dst_t
        a_ref[:, k * chan : (k + 1) * chan] = (mm(b, x) * rad).astype(BF16)


def rotate(b_ref, x, rad, a_ref):
    chan = x.shape[1]
    for k in range(b_ref.shape[0]):
        a_ref[:, k * chan : (k + 1) * chan] = (mm(b_ref[k], x) * rad).astype(BF16)


def mix(a_ref, w0, wr, wi, m_ref):
    kz, ko = w0.shape[0], wr.shape[0]
    m_ref[:, :kz] = mm(a_ref[:, :kz], w0[...]).astype(BF16)
    ap = a_ref[:, kz : kz + ko]
    am = a_ref[:, kz + ko :]
    m_ref[:, kz : kz + ko] = (mm(ap, wr[...]) - mm(am, wi[...])).astype(BF16)
    m_ref[:, kz + ko :] = (mm(ap, wi[...]) + mm(am, wr[...])).astype(BF16)


def back_to_nodes(t_ref, m_ref, chan):
    total = mm(t_ref[0], m_ref[:, :chan])
    for k in range(1, t_ref.shape[0]):
        total = total + mm(t_ref[k], m_ref[:, k * chan : (k + 1) * chan])
    return total


def gate(out, nat):
    o = out.reshape(-1, nat, out.shape[1])
    s = o[0]
    sig = jax.nn.sigmoid(s)
    h = jnp.concatenate([(s * sig)[None], o[1:] * sig[None]], axis=0)
    return h.reshape(out.shape)


def gate_back(dh, out, nat):
    o = out.reshape(-1, nat, out.shape[1])
    g = dh.reshape(o.shape)
    s = o[0]
    sig = jax.nn.sigmoid(s)
    slope = sig * (1.0 - sig)
    down = jnp.sum(g[1:] * o[1:], axis=0) * slope + g[0] * (sig + s * slope)
    d = jnp.concatenate([down[None], g[1:] * sig[None]], axis=0)
    return d.reshape(out.shape)


def pieces(kz, ko):
    first = kz * (kz // LANES)
    second = first + ko * (ko // LANES)
    return ((0, kz, kz // LANES), (first, ko, ko // LANES), (second, ko, ko // LANES))


def chunks(core):
    zhs, ys, cores, zls, xs = SIZES
    for y in range(ys):
        for zl in range(zls):
            for x in range(xs):
                for zh in range(zhs):
                    owner = (((zh * ys + y) * cores + core) * zls + zl) * xs + x
                    yield owner // 2, owner % 2, (y * zls + zl) * xs + x, zh


def unpack(core, mine, other, flat, stage):
    pair = flat.shape[0] // PAIRS
    part = (pair + 1) // 2
    where = [list(chunks(c)) for c in range(2)]
    first = lax.broadcasted_iota(jnp.int32, (part, LANES), 0) == 0
    for g in range(mine.shape[0]):
        m = mine[g].astype(F32)
        o = other[g].astype(F32)
        for c in range(2):
            stage[c] = jnp.where(core == c, m, o)
            for row, odd, sender, zh in where[c]:
                if sender != g:
                    continue
                block = stage[c, zh * part : (zh + 1) * part]
                to = row * pair + odd * (part - 1)
                if odd:
                    block = jnp.where(first, block + flat[to : to + part], block)
                flat[to : to + part] = block


def take_weights(flat, weights):
    for ref, (first, side, step) in zip(weights, pieces(weights[0].shape[0], weights[1].shape[0])):
        for q in range(step):
            ref[:, q * LANES : (q + 1) * LANES] = flat[pl.ds(first + q, side, stride=step), :].astype(BF16)


def put_grads(a_ref, dy_ref, kz, ko, flat):
    def put(grad, piece):
        first, side, step = piece
        for q in range(step):
            flat[pl.ds(first + q, side, stride=step), :] = grad[:, q * LANES : (q + 1) * LANES]

    p0, pr, pi = pieces(kz, ko)
    put(mm_at(a_ref[:, :kz], dy_ref[:, :kz]), p0)
    ap = a_ref[:, kz : kz + ko]
    am = a_ref[:, kz + ko :]
    dp = dy_ref[:, kz : kz + ko]
    dm = dy_ref[:, kz + ko :]
    put(mm_at(ap, dp) + mm_at(am, dm), pr)
    put(mm_at(ap, dm) - mm_at(am, dp), pi)


def pack(core, flat, stage, keep, send):
    pair = flat.shape[0] // PAIRS
    part = (pair + 1) // 2
    where = [list(chunks(c)) for c in range(2)]
    if stage.shape[1] > part * SIZES[0]:
        stage[...] = jnp.zeros_like(stage)
    for g in range(keep.shape[0]):
        for c in range(2):
            for row, odd, sender, zh in where[c]:
                if sender != g:
                    continue
                to = row * pair + odd * (part - 1)
                stage[c, zh * part : (zh + 1) * part] = flat[to : to + part]
        v0, v1 = stage[0], stage[1]
        keep[g] = jnp.where(core == 0, v0, v1).astype(BF16)
        send[g] = jnp.where(core == 0, v1, v0).astype(BF16)


def fetch(far, near, sems, i):
    return pltpu.make_async_copy(far, near, sems.at[i])


def first_kernel(nat, core_ref, mine, other, a0_ref, x_ref, dt_far, out_ref, h_ref,
                 flat, stage, w0, wr, wi, m_ref, dt_ref, sems):
    move = fetch(dt_far, dt_ref, sems, 0)
    move.start()
    unpack(core_ref[0], mine, other, flat, stage)
    take_weights(flat, (w0, wr, wi))
    mix(a0_ref, w0, wr, wi, m_ref)
    move.wait()
    out = x_ref[...].astype(F32) + back_to_nodes(dt_ref, m_ref, x_ref.shape[1]) / AVG
    out_ref[...] = out
    h_ref[...] = gate(out, nat).astype(BF16)


def second_kernel(nat, core_ref, mine, other, h_ref, cot_ref, rad_ref, b_far, dt_far, d_far,
                  keep, send, dy_ref, dout_ref, w0, wr, wi,
                  flat, stage, a_ref, m_ref, b_ref, dt_ref, d_ref, sems):
    chan = h_ref.shape[1]
    kz, ko = w0.shape[0], wr.shape[0]
    move_b = fetch(b_far, b_ref, sems, 0)
    move_dt = fetch(dt_far, dt_ref, sems, 1)
    move_d = fetch(d_far, d_ref, sems, 2)
    move_b.start()
    h1 = h_ref[...]
    unpack(core_ref[0], mine, other, flat, stage)
    take_weights(flat, (w0, wr, wi))
    move_b.wait()
    move_dt.start()
    rotate(b_ref, h1, rad_ref[...].astype(F32), a_ref)
    mix(a_ref, w0, wr, wi, m_ref)
    move_dt.wait()
    move_d.start()
    out2 = h1.astype(F32) + back_to_nodes(dt_ref, m_ref, chan) / AVG
    dout = gate_back(cot_ref[...].astype(F32), out2, nat)
    dout_ref[...] = dout
    dagg = (dout / AVG).astype(BF16)
    move_d.wait()
    for k in range(d_ref.shape[0]):
        dy_ref[:, k * chan : (k + 1) * chan] = mm(d_ref[k], dagg).astype(BF16)
    put_grads(a_ref, dy_ref, kz, ko, flat)
    pack(core_ref[0], flat, stage, keep, send)


def third_kernel(nat, core_ref, dy1_ref, dout_ref, w0, wr, wi, out_ref, a0_ref, rad_ref, bt_far, d_far,
                 keep, send, flat, stage, m_ref, dy_ref, bt_ref, d_ref, sems):
    chan = dout_ref.shape[1]
    kz, ko = w0.shape[0], wr.shape[0]
    move_bt = fetch(bt_far, bt_ref, sems, 0)
    move_d = fetch(d_far, d_ref, sems, 1)
    move_bt.start()
    rad = rad_ref[...].astype(F32)
    dp = dy1_ref[:, kz : kz + ko]
    dm = dy1_ref[:, kz + ko :]
    parts = (
        mm_bt(dy1_ref[:, :kz], w0[...]),
        mm_bt(dp, wr[...]) + mm_bt(dm, wi[...]),
        mm_bt(dm, wr[...]) - mm_bt(dp, wi[...]),
    )
    at = 0
    for part in parts:
        for q in range(part.shape[1] // chan):
            piece = part[:, q * chan : (q + 1) * chan].astype(BF16).astype(F32)
            m_ref[:, at : at + chan] = (piece * rad).astype(BF16)
            at += chan
    move_bt.wait()
    move_d.start()
    dh1 = (dout_ref[...] + back_to_nodes(bt_ref, m_ref, chan)).astype(BF16).astype(F32)
    dagg1 = (gate_back(dh1, out_ref[...], nat) / AVG).astype(BF16)
    move_d.wait()
    for k in range(d_ref.shape[0]):
        dy_ref[:, k * chan : (k + 1) * chan] = mm(d_ref[k], dagg1).astype(BF16)
    put_grads(a0_ref, dy_ref, kz, ko, flat)
    pack(core_ref[0], flat, stage, keep, send)


def sds(shape, dtype):
    return jax.ShapeDtypeStruct(shape, dtype)


def call(kernel, outs, args, scratch=(), scalars=0, far=0, flops=1 << 32, vmem=28 << 20):
    specs = [pl.BlockSpec(memory_space=pltpu.SMEM)] * scalars
    specs += [pl.BlockSpec(memory_space=pltpu.VMEM)] * (len(args) - scalars - far)
    specs += [pl.BlockSpec(memory_space=pl.ANY)] * far
    return pl.pallas_call(
        kernel,
        out_shape=outs,
        in_specs=specs,
        out_specs=[pl.BlockSpec(memory_space=pltpu.VMEM)] * len(outs),
        scratch_shapes=scratch,
        compiler_params=pltpu.CompilerParams(vmem_limit_bytes=vmem),
        cost_estimate=pl.CostEstimate(flops=flops, bytes_accessed=1 << 20, transcendentals=0),
    )(*args)


def count_of(axes):
    n = 1
    for a in axes:
        n *= lax.axis_size(a)
    return n


def from_everyone(x, axes):
    spread = jnp.broadcast_to(x[None], (count_of(axes), *x.shape))
    return lax.all_to_all(spread, axes, 0, 0, tiled=True)


def swap_core(x):
    return lax.ppermute(x, "core", [(0, 1), (1, 0)])


def local(node_feats, cotangent, wigner, radial, edge_src, edge_dst, edge_count, params, moment1, moment2):
    nat, coef, chan = node_feats.shape
    rows, _, edges = wigner.shape
    lone = (rows + 2) // 3
    kz, ko = lone * chan, (lone - 1) * chan
    layers, shard = params.shape
    far, near = count_of(FAR), count_of(NEAR)
    core = lax.axis_index("core").astype(jnp.int32).reshape(1)
    odd = lax.axis_index("x") % 2 == 1
    part = (shard + LANES // 2) // LANES
    spare = part * LANES - shard

    half = params.astype(BF16)
    half = jnp.where(odd, jnp.pad(half, ((0, 0), (spare, 0))), jnp.pad(half, ((0, 0), (0, spare))))
    block = -(-far * part // 8) * 8
    got = from_everyone(half.reshape(layers * part, LANES), FAR).reshape(far, layers, part, LANES)
    mine, other = [], []
    for i in range(layers):
        rows_i = jnp.pad(got[:, i].reshape(far * part, LANES), ((0, block - far * part), (0, 0)))
        mine.append(from_everyone(rows_i, NEAR))
        other.append(swap_core(mine[i]))

    x = jnp.transpose(node_feats, (1, 0, 2)).reshape(coef * nat, chan)
    cot = jnp.transpose(cotangent, (1, 0, 2)).reshape(coef * nat, chan)
    live = jnp.arange(edges, dtype=jnp.int32) < edge_count[0]
    dst = jnp.where(live, edge_dst, -1)
    wide = coef * nat
    mats = [sds((rows, edges, wide), BF16), sds((rows, wide, edges), BF16)] * 2
    act = sds((edges, rows * chan), BF16)
    a0, b, bt, d, dt = call(
        functools.partial(prep_kernel, nat),
        [act, *mats],
        (wigner, edge_src.reshape(1, edges), dst.reshape(1, edges), edge_src.reshape(edges, 1), dst.reshape(edges, 1), x, radial[0]),
        vmem=24 << 20,
    )
    flat = [pltpu.VMEM(((kz * kz + 2 * ko * ko) // LANES, LANES), F32), pltpu.VMEM((2, block, LANES), F32)]
    sides = [(kz, kz), (ko, ko), (ko, ko)]
    weights = [pltpu.VMEM(side, BF16) for side in sides]
    space = pltpu.VMEM((edges, rows * chan), BF16)
    tall, long = [pltpu.VMEM(m.shape, m.dtype) for m in mats[:2]]
    halves = [sds((near, block, LANES), BF16)] * 2
    node32, node16 = sds((wide, chan), F32), sds((wide, chan), BF16)

    def done(n):
        return pltpu.SemaphoreType.DMA((n,))

    out1, h1 = call(
        functools.partial(first_kernel, nat),
        [node32, node16],
        (core, mine[0], other[0], a0, x, dt),
        [*flat, *weights, space, long, done(1)],
        scalars=1,
        far=1,
        vmem=24 << 20,
    )
    keep1, send1, dy1, dout, *w1 = call(
        functools.partial(second_kernel, nat),
        [*halves, act, node32, *[sds(side, BF16) for side in sides]],
        (core, mine[1], other[1], h1, cot, radial[1], b, dt, d),
        [*flat, space, space, tall, long, tall, done(3)],
        scalars=1,
        far=3,
        vmem=36 << 20,
    )

    def chip_sum(keep, send):
        return (keep.astype(F32) + swap_core(send).astype(F32)).astype(BF16)

    def near_sum_of(pair):
        return lax.all_to_all(pair, NEAR, 0, 0, tiled=True).astype(F32).sum(axis=0)

    pair1 = chip_sum(keep1, send1)
    sum1 = near_sum_of(pair1)
    keep0, send0 = call(
        functools.partial(third_kernel, nat),
        halves,
        (core, dy1, dout, *w1, out1, a0, radial[1], bt, d),
        [*flat, space, space, long, tall, done(2)],
        scalars=1,
        far=2,
        vmem=32 << 20,
    )
    pair0 = chip_sum(keep0, send0)
    sum0 = near_sum_of(pair0)
    sums = [v[: far * part].reshape(far, part, LANES) for v in (sum0, sum1)]
    near_sum = jnp.concatenate(sums, axis=1)
    grad = lax.all_to_all(near_sum, FAR, 0, 0, tiled=True).sum(axis=0).reshape(layers, part * LANES)
    grad = jnp.where(odd, grad[:, spare:], grad[:, :shard])

    new_moment1 = 0.9 * moment1 + 0.1 * grad
    new_moment2 = 0.95 * moment2 + 0.05 * grad * grad
    m_hat = new_moment1 / (1.0 - 0.9**60)
    v_hat = new_moment2 / (1.0 - 0.95**60)
    new_params = params - 0.01 * (m_hat / (jnp.sqrt(v_hat) + 1e-08) + 0.1 * params)
    return (new_params, new_moment1, new_moment2)


def solution(mesh):
    fine = Mesh(mesh.devices.reshape(SIZES), AXES)
    flat = P(None, AXES)
    return jax.shard_map(
        local,
        mesh=fine,
        in_specs=(
            P(AXES, None, None),
            P(AXES, None, None),
            P(None, None, AXES),
            P(None, AXES, None),
            P(AXES),
            P(AXES),
            P(AXES),
            flat,
            flat,
            flat,
        ),
        out_specs=(flat, flat, flat),
        check_vma=False,
    )
```

```python
import functools

import jax
import jax.numpy as jnp
from jax import lax
from jax.experimental import pallas as pl
from jax.experimental.pallas import tpu as pltpu
from jax.sharding import Mesh
from jax.sharding import PartitionSpec as P

F32 = jnp.float32
BF16 = jnp.bfloat16
AVG = 10
AXES = ("zh", "y", "core", "zl", "x")
SIZES = (4, 4, 2, 2, 4)
NEAR = ("y", "zl", "x")
FAR = ("zh",)
LANES = 128


def mm(a, b):
    return lax.dot_general(a, b, (((1,), (0,)), ((), ())), preferred_element_type=F32)


def mm_bt(a, b):
    return lax.dot_general(a, b, (((1,), (1,)), ((), ())), preferred_element_type=F32)


def mm_at(a, b):
    return lax.dot_general(a, b, (((0,), (0,)), ((), ())), preferred_element_type=F32)


def prep_kernel(nat, wig_ref, src_ref, dst_ref, srcc_ref, dstc_ref, x_ref, rad_ref, a_ref, b_ref, bt_ref, d_ref, dt_ref):
    rows, coef, edges = wig_ref.shape
    wide = coef * nat
    chan = x_ref.shape[1]
    lane = lax.broadcasted_iota(jnp.int32, (coef, wide), 1)
    start = lax.broadcasted_iota(jnp.int32, (coef, wide), 0) * nat
    spread = ((lane >= start) & (lane < start + nat)).astype(BF16)
    lane_e = lax.broadcasted_iota(jnp.int32, (edges, wide), 1) % nat
    row_e = lax.broadcasted_iota(jnp.int32, (wide, edges), 0) % nat
    pick_src = (lane_e == srcc_ref[...]).astype(F32).astype(BF16)
    pick_dst = (lane_e == dstc_ref[...]).astype(F32).astype(BF16)
    pick_src_t = (row_e == src_ref[...]).astype(F32).astype(BF16)
    pick_dst_t = (row_e == dst_ref[...]).astype(F32).astype(BF16)
    x = x_ref[...]
    rad = rad_ref[...].astype(F32)
    for k in range(rows):
        w = wig_ref[k]
        e_wide = mm_at(w, spread).astype(BF16)
        wide_e = mm_at(spread, w).astype(BF16)
        b = e_wide * pick_src
        b_ref[k] = b
        d_ref[k] = e_wide * pick_dst
        bt_ref[k] = wide_e * pick_src_t
        dt_ref[k] = wide_e * pick_dst_t
        a_ref[:, k * chan : (k + 1) * chan] = (mm(b, x) * rad).astype(BF16)


def rotate(b_ref, x, rad, a_ref):
    chan = x.shape[1]
    for k in range(b_ref.shape[0]):
        a_ref[:, k * chan : (k + 1) * chan] = (mm(b_ref[k], x) * rad).astype(BF16)


def mix(a_ref, w0, wr, wi, m_ref):
    kz, ko = w0.shape[0], wr.shape[0]
    m_ref[:, :kz] = mm(a_ref[:, :kz], w0[...]).astype(BF16)
    ap = a_ref[:, kz : kz + ko]
    am = a_ref[:, kz + ko :]
    m_ref[:, kz : kz + ko] = (mm(ap, wr[...]) - mm(am, wi[...])).astype(BF16)
    m_ref[:, kz + ko :] = (mm(ap, wi[...]) + mm(am, wr[...])).astype(BF16)


def back_to_nodes(t_ref, m_ref, chan):
    total = mm(t_ref[0], m_ref[:, :chan])
    for k in range(1, t_ref.shape[0]):
        total = total + mm(t_ref[k], m_ref[:, k * chan : (k + 1) * chan])
    return total


def gate(out, nat):
    o = out.reshape(-1, nat, out.shape[1])
    s = o[0]
    sig = jax.nn.sigmoid(s)
    h = jnp.concatenate([(s * sig)[None], o[1:] * sig[None]], axis=0)
    return h.reshape(out.shape)


def gate_back(dh, out, nat):
    o = out.reshape(-1, nat, out.shape[1])
    g = dh.reshape(o.shape)
    s = o[0]
    sig = jax.nn.sigmoid(s)
    slope = sig * (1.0 - sig)
    down = jnp.sum(g[1:] * o[1:], axis=0) * slope + g[0] * (sig + s * slope)
    d = jnp.concatenate([down[None], g[1:] * sig[None]], axis=0)
    return d.reshape(out.shape)


def pieces(kz, ko):
    first = kz * (kz // LANES)
    second = first + ko * (ko // LANES)
    return ((0, kz, kz // LANES), (first, ko, ko // LANES), (second, ko, ko // LANES))


def chunks(core):
    zhs, ys, cores, zls, xs = SIZES
    for y in range(ys):
        for zl in range(zls):
            for x in range(xs):
                for zh in range(zhs):
                    owner = (((zh * ys + y) * cores + core) * zls + zl) * xs + x
                    yield owner // 2, owner % 2, (y * zls + zl) * xs + x, zh


def unpack(core, mine, other, flat, stage):
    layers = flat.shape[0]
    part = stage.shape[1] // (SIZES[0] * layers)
    pair = 2 * part - 1
    where = [list(chunks(c)) for c in range(2)]
    first = lax.broadcasted_iota(jnp.int32, (part, LANES), 0) == 0
    for g in range(mine.shape[0]):
        m = mine[g].astype(F32)
        o = other[g].astype(F32)
        for c in range(2):
            stage[c] = jnp.where(core == c, m, o)
            for row, odd, sender, zh in where[c]:
                if sender != g:
                    continue
                for i in range(layers):
                    at = (zh * layers + i) * part
                    block = stage[c, at : at + part]
                    to = row * pair + odd * (part - 1)
                    if odd:
                        block = jnp.where(first, block + flat[i, to : to + part], block)
                    flat[i, to : to + part] = block


def take_weights(flat, layer, weights):
    for ref, (first, side, step) in zip(weights, pieces(weights[0].shape[0], weights[1].shape[0])):
        for q in range(step):
            ref[:, q * LANES : (q + 1) * LANES] = flat[layer, pl.ds(first + q, side, stride=step), :].astype(BF16)


def put_grads(a_ref, dy_ref, kz, ko, layer, flat):
    def put(grad, piece):
        first, side, step = piece
        for q in range(step):
            flat[layer, pl.ds(first + q, side, stride=step), :] = grad[:, q * LANES : (q + 1) * LANES]

    p0, pr, pi = pieces(kz, ko)
    put(mm_at(a_ref[:, :kz], dy_ref[:, :kz]), p0)
    ap = a_ref[:, kz : kz + ko]
    am = a_ref[:, kz + ko :]
    dp = dy_ref[:, kz : kz + ko]
    dm = dy_ref[:, kz + ko :]
    put(mm_at(ap, dp) + mm_at(am, dm), pr)
    put(mm_at(ap, dm) - mm_at(am, dp), pi)


def pack(core, flat, stage, keep, send):
    layers = flat.shape[0]
    part = stage.shape[1] // (SIZES[0] * layers)
    pair = 2 * part - 1
    where = [list(chunks(c)) for c in range(2)]
    for g in range(keep.shape[0]):
        for c in range(2):
            for row, odd, sender, zh in where[c]:
                if sender != g:
                    continue
                for i in range(layers):
                    at = (zh * layers + i) * part
                    to = row * pair + odd * (part - 1)
                    stage[c, at : at + part] = flat[i, to : to + part]
        v0, v1 = stage[0], stage[1]
        keep[g] = jnp.where(core == 0, v0, v1).astype(BF16)
        send[g] = jnp.where(core == 0, v1, v0).astype(BF16)


def main_kernel(nat, core_ref, mine, other, a0_ref, x_ref, cot_ref, rad_ref, b_far, bt_far, d_far, dt_far,
                keep, send, flat, stage, w0, wr, wi, a_ref, m_ref, dy_ref, b_ref, bt_ref, d_ref, dt_ref, sems):
    moves = [
        pltpu.make_async_copy(far, near, sems.at[i])
        for i, (far, near) in enumerate(((dt_far, dt_ref), (b_far, b_ref), (d_far, d_ref), (bt_far, bt_ref)))
    ]
    moves[0].start()
    chan = x_ref.shape[1]
    rows = b_ref.shape[0]
    kz, ko = w0.shape[0], wr.shape[0]
    core = core_ref[0]
    rad = rad_ref[...].astype(F32)
    unpack(core, mine, other, flat, stage)
    moves[1].start()
    take_weights(flat, 0, (w0, wr, wi))
    mix(a0_ref, w0, wr, wi, m_ref)
    moves[0].wait()
    out1 = x_ref[...].astype(F32) + back_to_nodes(dt_ref, m_ref, chan) / AVG
    h1 = gate(out1, nat).astype(BF16)
    moves[1].wait()
    moves[2].start()
    rotate(b_ref, h1, rad, a_ref)
    take_weights(flat, 1, (w0, wr, wi))
    mix(a_ref, w0, wr, wi, m_ref)
    out2 = h1.astype(F32) + back_to_nodes(dt_ref, m_ref, chan) / AVG
    dout2 = gate_back(cot_ref[...].astype(F32), out2, nat)
    dagg = (dout2 / AVG).astype(BF16)
    moves[2].wait()
    moves[3].start()
    for k in range(rows):
        dy_ref[:, k * chan : (k + 1) * chan] = mm(d_ref[k], dagg).astype(BF16)
    put_grads(a_ref, dy_ref, kz, ko, 1, flat)
    dp = dy_ref[:, kz : kz + ko]
    dm = dy_ref[:, kz + ko :]
    parts = (
        mm_bt(dy_ref[:, :kz], w0[...]),
        mm_bt(dp, wr[...]) + mm_bt(dm, wi[...]),
        mm_bt(dm, wr[...]) - mm_bt(dp, wi[...]),
    )
    at = 0
    for part in parts:
        for q in range(part.shape[1] // chan):
            piece = part[:, q * chan : (q + 1) * chan].astype(BF16).astype(F32)
            m_ref[:, at : at + chan] = (piece * rad).astype(BF16)
            at += chan
    moves[3].wait()
    dh1 = (dout2 + back_to_nodes(bt_ref, m_ref, chan)).astype(BF16).astype(F32)
    dagg1 = (gate_back(dh1, out1, nat) / AVG).astype(BF16)
    for k in range(rows):
        dy_ref[:, k * chan : (k + 1) * chan] = mm(d_ref[k], dagg1).astype(BF16)
    put_grads(a0_ref, dy_ref, kz, ko, 0, flat)
    pack(core, flat, stage, keep, send)


def sds(shape, dtype):
    return jax.ShapeDtypeStruct(shape, dtype)


def call(kernel, outs, args, scratch=(), scalars=0, far=0, flops=1 << 32, vmem=28 << 20):
    specs = [pl.BlockSpec(memory_space=pltpu.SMEM)] * scalars
    specs += [pl.BlockSpec(memory_space=pltpu.VMEM)] * (len(args) - scalars - far)
    specs += [pl.BlockSpec(memory_space=pl.ANY)] * far
    return pl.pallas_call(
        kernel,
        out_shape=outs,
        in_specs=specs,
        out_specs=[pl.BlockSpec(memory_space=pltpu.VMEM)] * len(outs),
        scratch_shapes=scratch,
        compiler_params=pltpu.CompilerParams(vmem_limit_bytes=vmem),
        cost_estimate=pl.CostEstimate(flops=flops, bytes_accessed=1 << 20, transcendentals=0),
    )(*args)


def count_of(axes):
    n = 1
    for a in axes:
        n *= lax.axis_size(a)
    return n


def from_everyone(x, axes):
    spread = jnp.broadcast_to(x[None], (count_of(axes), *x.shape))
    return lax.all_to_all(spread, axes, 0, 0, tiled=True)


def swap_core(x):
    return lax.ppermute(x, "core", [(0, 1), (1, 0)])


def local(node_feats, cotangent, wigner, radial, edge_src, edge_dst, edge_count, params, moment1, moment2):
    nat, coef, chan = node_feats.shape
    rows, _, edges = wigner.shape
    lone = (rows + 2) // 3
    kz, ko = lone * chan, (lone - 1) * chan
    layers, shard = params.shape
    far, near = count_of(FAR), count_of(NEAR)
    core = lax.axis_index("core").astype(jnp.int32).reshape(1)
    odd = lax.axis_index("x") % 2 == 1
    part = (shard + LANES // 2) // LANES
    spare = part * LANES - shard

    half = params.astype(BF16)
    half = jnp.where(odd, jnp.pad(half, ((0, 0), (spare, 0))), jnp.pad(half, ((0, 0), (0, spare))))
    got = from_everyone(half.reshape(layers * part, LANES), FAR).reshape(far * layers * part, LANES)
    mine = from_everyone(got, NEAR)
    other = swap_core(mine)

    x = jnp.transpose(node_feats, (1, 0, 2)).reshape(coef * nat, chan)
    cot = jnp.transpose(cotangent, (1, 0, 2)).reshape(coef * nat, chan)
    live = jnp.arange(edges, dtype=jnp.int32) < edge_count[0]
    dst = jnp.where(live, edge_dst, -1)
    wide = coef * nat
    mats = [sds((rows, edges, wide), BF16), sds((rows, wide, edges), BF16)] * 2
    act = sds((edges, rows * chan), BF16)
    a0, b, bt, d, dt = call(
        functools.partial(prep_kernel, nat),
        [act, *mats],
        (wigner, edge_src.reshape(1, edges), dst.reshape(1, edges), edge_src.reshape(edges, 1), dst.reshape(edges, 1), x, radial[0]),
        vmem=24 << 20,
    )
    block = far * layers * part
    flat = [pltpu.VMEM((layers, (kz * kz + 2 * ko * ko) // LANES, LANES), F32), pltpu.VMEM((2, block, LANES), F32)]
    weights = [pltpu.VMEM((kz, kz), BF16), pltpu.VMEM((ko, ko), BF16), pltpu.VMEM((ko, ko), BF16)]
    space = pltpu.VMEM((edges, rows * chan), BF16)
    held = [pltpu.VMEM(m.shape, m.dtype) for m in mats]
    keep, send = call(
        functools.partial(main_kernel, nat),
        [sds((near, block, LANES), BF16)] * 2,
        (core, mine, other, a0, x, cot, radial[1], b, bt, d, dt),
        [*flat, *weights, space, space, space, *held, pltpu.SemaphoreType.DMA((len(held),))],
        scalars=1,
        far=len(held),
        vmem=44 << 20,
    )
    pair = (keep.astype(F32) + swap_core(send).astype(F32)).astype(BF16)
    arrived = lax.all_to_all(pair, NEAR, 0, 0, tiled=True)
    near_sum = arrived.astype(F32).sum(axis=0).reshape(far, layers * part, LANES)
    grad = lax.all_to_all(near_sum, FAR, 0, 0, tiled=True).sum(axis=0).reshape(layers, part * LANES)
    grad = jnp.where(odd, grad[:, spare:], grad[:, :shard])

    new_moment1 = 0.9 * moment1 + 0.1 * grad
    new_moment2 = 0.95 * moment2 + 0.05 * grad * grad
    m_hat = new_moment1 / (1.0 - 0.9**60)
    v_hat = new_moment2 / (1.0 - 0.95**60)
    new_params = params - 0.01 * (m_hat / (jnp.sqrt(v_hat) + 1e-08) + 0.1 * params)
    return (new_params, new_moment1, new_moment2)


def solution(mesh):
    fine = Mesh(mesh.devices.reshape(SIZES), AXES)
    flat = P(None, AXES)
    return jax.shard_map(
        local,
        mesh=fine,
        in_specs=(
            P(AXES, None, None),
            P(AXES, None, None),
            P(None, None, AXES),
            P(None, AXES, None),
            P(AXES),
            P(AXES),
            P(AXES),
            flat,
            flat,
            flat,
        ),
        out_specs=(flat, flat, flat),
        check_vma=False,
    )
```

```python
import functools

import jax
import jax.numpy as jnp
from jax import lax
from jax.experimental import pallas as pl
from jax.experimental.pallas import tpu as pltpu
from jax.sharding import Mesh
from jax.sharding import PartitionSpec as P

F32 = jnp.float32
BF16 = jnp.bfloat16
AVG = 10
AXES = ("zh", "y", "core", "zl", "x")
SIZES = (4, 4, 2, 2, 4)
NEAR = ("y", "zl")
FAR = ("zh", "x")
LANES = 128


def mm(a, b):
    return lax.dot_general(a, b, (((1,), (0,)), ((), ())), preferred_element_type=F32)


def mm_bt(a, b):
    return lax.dot_general(a, b, (((1,), (1,)), ((), ())), preferred_element_type=F32)


def mm_at(a, b):
    return lax.dot_general(a, b, (((0,), (0,)), ((), ())), preferred_element_type=F32)


def prep_kernel(nat, wig_ref, src_ref, dst_ref, srcc_ref, dstc_ref, x_ref, rad_ref, a_ref, b_ref, bt_ref, d_ref, dt_ref):
    rows, coef, edges = wig_ref.shape
    wide = coef * nat
    chan = x_ref.shape[1]
    lane = lax.broadcasted_iota(jnp.int32, (coef, wide), 1)
    start = lax.broadcasted_iota(jnp.int32, (coef, wide), 0) * nat
    spread = ((lane >= start) & (lane < start + nat)).astype(BF16)
    lane_e = lax.broadcasted_iota(jnp.int32, (edges, wide), 1) % nat
    row_e = lax.broadcasted_iota(jnp.int32, (wide, edges), 0) % nat
    pick_src = (lane_e == srcc_ref[...]).astype(F32).astype(BF16)
    pick_dst = (lane_e == dstc_ref[...]).astype(F32).astype(BF16)
    pick_src_t = (row_e == src_ref[...]).astype(F32).astype(BF16)
    pick_dst_t = (row_e == dst_ref[...]).astype(F32).astype(BF16)
    x = x_ref[...]
    rad = rad_ref[...].astype(F32)
    for k in range(rows):
        w = wig_ref[k]
        e_wide = mm_at(w, spread).astype(BF16)
        wide_e = mm_at(spread, w).astype(BF16)
        b = e_wide * pick_src
        b_ref[k] = b
        d_ref[k] = e_wide * pick_dst
        bt_ref[k] = wide_e * pick_src_t
        dt_ref[k] = wide_e * pick_dst_t
        a_ref[:, k * chan : (k + 1) * chan] = (mm(b, x) * rad).astype(BF16)


def rotate(b_ref, x, rad, a_ref):
    chan = x.shape[1]
    for k in range(b_ref.shape[0]):
        a_ref[:, k * chan : (k + 1) * chan] = (mm(b_ref[k], x) * rad).astype(BF16)


def mix(a_ref, w0, wr, wi, m_ref):
    kz, ko = w0.shape[0], wr.shape[0]
    m_ref[:, :kz] = mm(a_ref[:, :kz], w0[...]).astype(BF16)
    ap = a_ref[:, kz : kz + ko]
    am = a_ref[:, kz + ko :]
    m_ref[:, kz : kz + ko] = (mm(ap, wr[...]) - mm(am, wi[...])).astype(BF16)
    m_ref[:, kz + ko :] = (mm(ap, wi[...]) + mm(am, wr[...])).astype(BF16)


def back_to_nodes(t_ref, m_ref, chan):
    total = mm(t_ref[0], m_ref[:, :chan])
    for k in range(1, t_ref.shape[0]):
        total = total + mm(t_ref[k], m_ref[:, k * chan : (k + 1) * chan])
    return total


def gate(out, nat):
    o = out.reshape(-1, nat, out.shape[1])
    s = o[0]
    sig = jax.nn.sigmoid(s)
    h = jnp.concatenate([(s * sig)[None], o[1:] * sig[None]], axis=0)
    return h.reshape(out.shape)


def gate_back(dh, out, nat):
    o = out.reshape(-1, nat, out.shape[1])
    g = dh.reshape(o.shape)
    s = o[0]
    sig = jax.nn.sigmoid(s)
    slope = sig * (1.0 - sig)
    down = jnp.sum(g[1:] * o[1:], axis=0) * slope + g[0] * (sig + s * slope)
    d = jnp.concatenate([down[None], g[1:] * sig[None]], axis=0)
    return d.reshape(out.shape)


def pieces(kz, ko):
    first = kz * (kz // LANES)
    second = first + ko * (ko // LANES)
    return ((0, kz, kz // LANES), (first, ko, ko // LANES), (second, ko, ko // LANES))


def chunk_at(g, core, zh):
    y, zl = divmod(g, SIZES[3])
    return ((zh * SIZES[1] + y) * SIZES[2] + core) * SIZES[3] + zl


def unpack(core, mine, other, layer, flat, stage):
    rows = stage.shape[1]
    part = rows // SIZES[0]
    for g in range(mine.shape[0]):
        m = mine[g, layer * rows : (layer + 1) * rows].astype(F32)
        o = other[g, layer * rows : (layer + 1) * rows].astype(F32)
        for c in range(2):
            stage[c] = jnp.where(core == c, m, o)
            for zh in range(SIZES[0]):
                at = chunk_at(g, c, zh) * part
                flat[layer, at : at + part] = stage[c, zh * part : (zh + 1) * part]


def take_weights(flat, layer, weights):
    for ref, (first, side, step) in zip(weights, pieces(weights[0].shape[0], weights[1].shape[0])):
        for q in range(step):
            ref[:, q * LANES : (q + 1) * LANES] = flat[layer, pl.ds(first + q, side, stride=step), :].astype(BF16)


def put_grads(a_ref, dy_ref, kz, ko, layer, flat):
    def put(grad, piece):
        first, side, step = piece
        for q in range(step):
            flat[layer, pl.ds(first + q, side, stride=step), :] = grad[:, q * LANES : (q + 1) * LANES]

    p0, pr, pi = pieces(kz, ko)
    put(mm_at(a_ref[:, :kz], dy_ref[:, :kz]), p0)
    ap = a_ref[:, kz : kz + ko]
    am = a_ref[:, kz + ko :]
    dp = dy_ref[:, kz : kz + ko]
    dm = dy_ref[:, kz + ko :]
    put(mm_at(ap, dp) + mm_at(am, dm), pr)
    put(mm_at(ap, dm) - mm_at(am, dp), pi)


def pack(core, layer, flat, stage, keep, send):
    rows = stage.shape[1]
    part = rows // SIZES[0]
    for g in range(keep.shape[0]):
        for c in range(2):
            for zh in range(SIZES[0]):
                at = chunk_at(g, c, zh) * part
                stage[c, zh * part : (zh + 1) * part] = flat[layer, at : at + part]
        v0, v1 = stage[0], stage[1]
        keep[g, layer * rows : (layer + 1) * rows] = jnp.where(core == 0, v0, v1).astype(BF16)
        send[g, layer * rows : (layer + 1) * rows] = jnp.where(core == 0, v1, v0).astype(BF16)


def main_kernel(nat, core_ref, mine, other, a0_ref, x_ref, cot_ref, rad_ref, b_far, bt_far, d_far, dt_far,
                keep, send, flat, stage, w0, wr, wi, a_ref, m_ref, dy_ref, b_ref, bt_ref, d_ref, dt_ref, sems):
    moves = [
        pltpu.make_async_copy(far, near, sems.at[i])
        for i, (far, near) in enumerate(((dt_far, dt_ref), (b_far, b_ref), (d_far, d_ref), (bt_far, bt_ref)))
    ]
    moves[0].start()
    chan = x_ref.shape[1]
    rows = b_ref.shape[0]
    kz, ko = w0.shape[0], wr.shape[0]
    core = core_ref[0]
    rad = rad_ref[...].astype(F32)
    unpack(core, mine, other, 0, flat, stage)
    moves[1].start()
    take_weights(flat, 0, (w0, wr, wi))
    mix(a0_ref, w0, wr, wi, m_ref)
    moves[0].wait()
    out1 = x_ref[...].astype(F32) + back_to_nodes(dt_ref, m_ref, chan) / AVG
    h1 = gate(out1, nat).astype(BF16)
    moves[1].wait()
    moves[2].start()
    rotate(b_ref, h1, rad, a_ref)
    unpack(core, mine, other, 1, flat, stage)
    take_weights(flat, 1, (w0, wr, wi))
    mix(a_ref, w0, wr, wi, m_ref)
    out2 = h1.astype(F32) + back_to_nodes(dt_ref, m_ref, chan) / AVG
    dout2 = gate_back(cot_ref[...].astype(F32), out2, nat)
    dagg = (dout2 / AVG).astype(BF16)
    moves[2].wait()
    moves[3].start()
    for k in range(rows):
        dy_ref[:, k * chan : (k + 1) * chan] = mm(d_ref[k], dagg).astype(BF16)
    put_grads(a_ref, dy_ref, kz, ko, 1, flat)
    pack(core, 1, flat, stage, keep, send)
    dp = dy_ref[:, kz : kz + ko]
    dm = dy_ref[:, kz + ko :]
    parts = (
        mm_bt(dy_ref[:, :kz], w0[...]),
        mm_bt(dp, wr[...]) + mm_bt(dm, wi[...]),
        mm_bt(dm, wr[...]) - mm_bt(dp, wi[...]),
    )
    at = 0
    for part in parts:
        for q in range(part.shape[1] // chan):
            piece = part[:, q * chan : (q + 1) * chan].astype(BF16).astype(F32)
            m_ref[:, at : at + chan] = (piece * rad).astype(BF16)
            at += chan
    moves[3].wait()
    dh1 = (dout2 + back_to_nodes(bt_ref, m_ref, chan)).astype(BF16).astype(F32)
    dagg1 = (gate_back(dh1, out1, nat) / AVG).astype(BF16)
    for k in range(rows):
        dy_ref[:, k * chan : (k + 1) * chan] = mm(d_ref[k], dagg1).astype(BF16)
    put_grads(a0_ref, dy_ref, kz, ko, 0, flat)
    pack(core, 0, flat, stage, keep, send)


def sds(shape, dtype):
    return jax.ShapeDtypeStruct(shape, dtype)


def call(kernel, outs, args, scratch=(), scalars=0, far=0, flops=1 << 32, vmem=28 << 20):
    specs = [pl.BlockSpec(memory_space=pltpu.SMEM)] * scalars
    specs += [pl.BlockSpec(memory_space=pltpu.VMEM)] * (len(args) - scalars - far)
    specs += [pl.BlockSpec(memory_space=pl.ANY)] * far
    return pl.pallas_call(
        kernel,
        out_shape=outs,
        in_specs=specs,
        out_specs=[pl.BlockSpec(memory_space=pltpu.VMEM)] * len(outs),
        scratch_shapes=scratch,
        compiler_params=pltpu.CompilerParams(vmem_limit_bytes=vmem),
        cost_estimate=pl.CostEstimate(flops=flops, bytes_accessed=1 << 20, transcendentals=0),
    )(*args)


def count_of(axes):
    n = 1
    for a in axes:
        n *= lax.axis_size(a)
    return n


def from_everyone(x, axes):
    spread = jnp.broadcast_to(x[None], (count_of(axes), *x.shape))
    return lax.all_to_all(spread, axes, 0, 0, tiled=True)


def swap_core(x):
    return lax.ppermute(x, "core", [(0, 1), (1, 0)])


def local(node_feats, cotangent, wigner, radial, edge_src, edge_dst, edge_count, params, moment1, moment2):
    nat, coef, chan = node_feats.shape
    rows, _, edges = wigner.shape
    lone = (rows + 2) // 3
    kz, ko = lone * chan, (lone - 1) * chan
    layers, shard = params.shape
    far, near = count_of(FAR), count_of(NEAR)
    core = lax.axis_index("core").astype(jnp.int32).reshape(1)
    block = far * shard // LANES
    lines = layers * shard // LANES

    got = from_everyone(params.astype(BF16).reshape(lines, LANES), FAR).reshape(far, layers, shard)
    got = jnp.moveaxis(got, 1, 0).reshape(layers * block, LANES)
    mine = from_everyone(got, NEAR)
    other = swap_core(mine)

    x = jnp.transpose(node_feats, (1, 0, 2)).reshape(coef * nat, chan)
    cot = jnp.transpose(cotangent, (1, 0, 2)).reshape(coef * nat, chan)
    live = jnp.arange(edges, dtype=jnp.int32) < edge_count[0]
    dst = jnp.where(live, edge_dst, -1)
    wide = coef * nat
    mats = [sds((rows, edges, wide), BF16), sds((rows, wide, edges), BF16)] * 2
    act = sds((edges, rows * chan), BF16)
    a0, b, bt, d, dt = call(
        functools.partial(prep_kernel, nat),
        [act, *mats],
        (wigner, edge_src.reshape(1, edges), dst.reshape(1, edges), edge_src.reshape(edges, 1), dst.reshape(edges, 1), x, radial[0]),
        vmem=24 << 20,
    )
    flat = [pltpu.VMEM((layers, (kz * kz + 2 * ko * ko) // LANES, LANES), F32), pltpu.VMEM((2, block, LANES), F32)]
    weights = [pltpu.VMEM((kz, kz), BF16), pltpu.VMEM((ko, ko), BF16), pltpu.VMEM((ko, ko), BF16)]
    space = pltpu.VMEM((edges, rows * chan), BF16)
    held = [pltpu.VMEM(m.shape, m.dtype) for m in mats]
    keep, send = call(
        functools.partial(main_kernel, nat),
        [sds((near, layers * block, LANES), BF16)] * 2,
        (core, mine, other, a0, x, cot, radial[1], b, bt, d, dt),
        [*flat, *weights, space, space, space, *held, pltpu.SemaphoreType.DMA((len(held),))],
        scalars=1,
        far=len(held),
        vmem=44 << 20,
    )
    pair = (keep.astype(F32) + swap_core(send).astype(F32)).astype(BF16)
    arrived = lax.all_to_all(pair, NEAR, 0, 0, tiled=True)
    near_sum = arrived.astype(F32).sum(axis=0).astype(BF16).reshape(layers, far, shard)
    near_sum = jnp.moveaxis(near_sum, 1, 0).reshape(far, lines, LANES)
    grad = lax.all_to_all(near_sum, FAR, 0, 0, tiled=True).astype(F32).sum(axis=0).reshape(layers, shard)

    new_moment1 = 0.9 * moment1 + 0.1 * grad
    new_moment2 = 0.95 * moment2 + 0.05 * grad * grad
    m_hat = new_moment1 / (1.0 - 0.9**60)
    v_hat = new_moment2 / (1.0 - 0.95**60)
    new_params = params - 0.01 * (m_hat / (jnp.sqrt(v_hat) + 1e-08) + 0.1 * params)
    return (new_params, new_moment1, new_moment2)


def solution(mesh):
    fine = Mesh(mesh.devices.reshape(SIZES), AXES)
    flat = P(None, AXES)
    return jax.shard_map(
        local,
        mesh=fine,
        in_specs=(
            P(AXES, None, None),
            P(AXES, None, None),
            P(None, None, AXES),
            P(None, AXES, None),
            P(AXES),
            P(AXES),
            P(AXES),
            flat,
            flat,
            flat,
        ),
        out_specs=(flat, flat, flat),
        check_vma=False,
    )
```

```python
import functools

import jax
import jax.numpy as jnp
from jax import lax
from jax.experimental import pallas as pl
from jax.experimental.pallas import tpu as pltpu
from jax.sharding import Mesh
from jax.sharding import PartitionSpec as P

F32 = jnp.float32
BF16 = jnp.bfloat16
AVG = 10
AXES = ("zh", "y", "core", "zl", "x")
SIZES = (4, 4, 2, 2, 4)
NEAR = ("y", "zl", "x")
FAR = ("zh",)
LANES = 128


def mm(a, b):
    return lax.dot_general(a, b, (((1,), (0,)), ((), ())), preferred_element_type=F32)


def mm_bt(a, b):
    return lax.dot_general(a, b, (((1,), (1,)), ((), ())), preferred_element_type=F32)


def mm_at(a, b):
    return lax.dot_general(a, b, (((0,), (0,)), ((), ())), preferred_element_type=F32)


def prep_kernel(nat, wig_ref, src_ref, dst_ref, srcc_ref, dstc_ref, x_ref, rad_ref, a_ref, b_ref, bt_ref, d_ref, dt_ref):
    rows, coef, edges = wig_ref.shape
    wide = coef * nat
    chan = x_ref.shape[1]
    lane = lax.broadcasted_iota(jnp.int32, (coef, wide), 1)
    start = lax.broadcasted_iota(jnp.int32, (coef, wide), 0) * nat
    spread = ((lane >= start) & (lane < start + nat)).astype(BF16)
    lane_e = lax.broadcasted_iota(jnp.int32, (edges, wide), 1) % nat
    row_e = lax.broadcasted_iota(jnp.int32, (wide, edges), 0) % nat
    pick_src = (lane_e == srcc_ref[...]).astype(F32).astype(BF16)
    pick_dst = (lane_e == dstc_ref[...]).astype(F32).astype(BF16)
    pick_src_t = (row_e == src_ref[...]).astype(F32).astype(BF16)
    pick_dst_t = (row_e == dst_ref[...]).astype(F32).astype(BF16)
    x = x_ref[...]
    rad = rad_ref[...].astype(F32)
    for k in range(rows):
        w = wig_ref[k]
        e_wide = mm_at(w, spread).astype(BF16)
        wide_e = mm_at(spread, w).astype(BF16)
        b = e_wide * pick_src
        b_ref[k] = b
        d_ref[k] = e_wide * pick_dst
        bt_ref[:, k * edges : (k + 1) * edges] = wide_e * pick_src_t
        dt_ref[:, k * edges : (k + 1) * edges] = wide_e * pick_dst_t
        a_ref[:, k * chan : (k + 1) * chan] = (mm(b, x) * rad).astype(BF16)


def rotate(b_ref, x, rad, a_ref):
    chan = x.shape[1]
    for k in range(b_ref.shape[0]):
        a_ref[:, k * chan : (k + 1) * chan] = (mm(b_ref[k], x) * rad).astype(BF16)


def by_row(value, first, chan, m_ref):
    edges = value.shape[0]
    for q in range(value.shape[1] // chan):
        m_ref[(first + q) * edges : (first + q + 1) * edges] = value[:, q * chan : (q + 1) * chan].astype(BF16)


def mix(a_ref, w0, wr, wi, m_ref):
    kz, ko = w0.shape[0], wr.shape[0]
    chan = m_ref.shape[1]
    by_row(mm(a_ref[:, :kz], w0[...]), 0, chan, m_ref)
    ap = a_ref[:, kz : kz + ko]
    am = a_ref[:, kz + ko :]
    by_row(mm(ap, wr[...]) - mm(am, wi[...]), kz // chan, chan, m_ref)
    by_row(mm(ap, wi[...]) + mm(am, wr[...]), (kz + ko) // chan, chan, m_ref)


def back_to_nodes(t_ref, m_ref):
    return mm(t_ref[...], m_ref[...])


def gate(out, nat):
    o = out.reshape(-1, nat, out.shape[1])
    s = o[0]
    sig = jax.nn.sigmoid(s)
    h = jnp.concatenate([(s * sig)[None], o[1:] * sig[None]], axis=0)
    return h.reshape(out.shape)


def gate_back(dh, out, nat):
    o = out.reshape(-1, nat, out.shape[1])
    g = dh.reshape(o.shape)
    s = o[0]
    sig = jax.nn.sigmoid(s)
    slope = sig * (1.0 - sig)
    down = jnp.sum(g[1:] * o[1:], axis=0) * slope + g[0] * (sig + s * slope)
    d = jnp.concatenate([down[None], g[1:] * sig[None]], axis=0)
    return d.reshape(out.shape)


def pieces(kz, ko):
    first = kz * (kz // LANES)
    second = first + ko * (ko // LANES)
    return ((0, kz, kz // LANES), (first, ko, ko // LANES), (second, ko, ko // LANES))


def chunks(core):
    zhs, ys, cores, zls, xs = SIZES
    for y in range(ys):
        for zl in range(zls):
            for x in range(xs):
                for zh in range(zhs):
                    owner = (((zh * ys + y) * cores + core) * zls + zl) * xs + x
                    yield owner // 2, owner % 2, (y * zls + zl) * xs + x, zh


def unpack(core, mine, other, flat, stage):
    layers = flat.shape[0]
    part = stage.shape[1] // (SIZES[0] * layers)
    pair = 2 * part - 1
    where = [list(chunks(c)) for c in range(2)]
    first = lax.broadcasted_iota(jnp.int32, (part, LANES), 0) == 0
    for g in range(mine.shape[0]):
        m = mine[g].astype(F32)
        o = other[g].astype(F32)
        for c in range(2):
            stage[c] = jnp.where(core == c, m, o)
            for row, odd, sender, zh in where[c]:
                if sender != g:
                    continue
                for i in range(layers):
                    at = (zh * layers + i) * part
                    block = stage[c, at : at + part]
                    to = row * pair + odd * (part - 1)
                    if odd:
                        block = jnp.where(first, block + flat[i, to : to + part], block)
                    flat[i, to : to + part] = block


def take_weights(flat, layer, weights):
    for ref, (first, side, step) in zip(weights, pieces(weights[0].shape[0], weights[1].shape[0])):
        for q in range(step):
            ref[:, q * LANES : (q + 1) * LANES] = flat[layer, pl.ds(first + q, side, stride=step), :].astype(BF16)


def put_grads(a_ref, dy_ref, kz, ko, layer, flat):
    def put(grad, piece):
        first, side, step = piece
        for q in range(step):
            flat[layer, pl.ds(first + q, side, stride=step), :] = grad[:, q * LANES : (q + 1) * LANES]

    p0, pr, pi = pieces(kz, ko)
    put(mm_at(a_ref[:, :kz], dy_ref[:, :kz]), p0)
    ap = a_ref[:, kz : kz + ko]
    am = a_ref[:, kz + ko :]
    dp = dy_ref[:, kz : kz + ko]
    dm = dy_ref[:, kz + ko :]
    put(mm_at(ap, dp) + mm_at(am, dm), pr)
    put(mm_at(ap, dm) - mm_at(am, dp), pi)


def pack(core, flat, stage, keep, send):
    layers = flat.shape[0]
    part = stage.shape[1] // (SIZES[0] * layers)
    pair = 2 * part - 1
    where = [list(chunks(c)) for c in range(2)]
    for g in range(keep.shape[0]):
        for c in range(2):
            for row, odd, sender, zh in where[c]:
                if sender != g:
                    continue
                for i in range(layers):
                    at = (zh * layers + i) * part
                    to = row * pair + odd * (part - 1)
                    stage[c, at : at + part] = flat[i, to : to + part]
        v0, v1 = stage[0], stage[1]
        keep[g] = jnp.where(core == 0, v0, v1).astype(BF16)
        send[g] = jnp.where(core == 0, v1, v0).astype(BF16)


def main_kernel(nat, core_ref, mine, other, a0_ref, x_ref, cot_ref, rad_ref, b_far, bt_far, d_far, dt_far,
                keep, send, flat, stage, w0, wr, wi, a_ref, m_ref, dy_ref, b_ref, bt_ref, d_ref, dt_ref, sems):
    moves = [
        pltpu.make_async_copy(far, near, sems.at[i])
        for i, (far, near) in enumerate(((dt_far, dt_ref), (b_far, b_ref), (d_far, d_ref), (bt_far, bt_ref)))
    ]
    moves[0].start()
    chan = x_ref.shape[1]
    rows = b_ref.shape[0]
    kz, ko = w0.shape[0], wr.shape[0]
    core = core_ref[0]
    rad = rad_ref[...].astype(F32)
    unpack(core, mine, other, flat, stage)
    moves[1].start()
    take_weights(flat, 0, (w0, wr, wi))
    mix(a0_ref, w0, wr, wi, m_ref)
    moves[0].wait()
    out1 = x_ref[...].astype(F32) + back_to_nodes(dt_ref, m_ref) / AVG
    h1 = gate(out1, nat).astype(BF16)
    moves[1].wait()
    moves[2].start()
    rotate(b_ref, h1, rad, a_ref)
    take_weights(flat, 1, (w0, wr, wi))
    mix(a_ref, w0, wr, wi, m_ref)
    out2 = h1.astype(F32) + back_to_nodes(dt_ref, m_ref) / AVG
    dout2 = gate_back(cot_ref[...].astype(F32), out2, nat)
    dagg = (dout2 / AVG).astype(BF16)
    moves[2].wait()
    moves[3].start()
    for k in range(rows):
        dy_ref[:, k * chan : (k + 1) * chan] = mm(d_ref[k], dagg).astype(BF16)
    put_grads(a_ref, dy_ref, kz, ko, 1, flat)
    dp = dy_ref[:, kz : kz + ko]
    dm = dy_ref[:, kz + ko :]
    parts = (
        mm_bt(dy_ref[:, :kz], w0[...]),
        mm_bt(dp, wr[...]) + mm_bt(dm, wi[...]),
        mm_bt(dm, wr[...]) - mm_bt(dp, wi[...]),
    )
    at = 0
    for part in parts:
        for q in range(part.shape[1] // chan):
            piece = part[:, q * chan : (q + 1) * chan].astype(BF16).astype(F32)
            by_row(piece * rad, at, chan, m_ref)
            at += 1
    moves[3].wait()
    dh1 = (dout2 + back_to_nodes(bt_ref, m_ref)).astype(BF16).astype(F32)
    dagg1 = (gate_back(dh1, out1, nat) / AVG).astype(BF16)
    for k in range(rows):
        dy_ref[:, k * chan : (k + 1) * chan] = mm(d_ref[k], dagg1).astype(BF16)
    put_grads(a0_ref, dy_ref, kz, ko, 0, flat)
    pack(core, flat, stage, keep, send)


def sds(shape, dtype):
    return jax.ShapeDtypeStruct(shape, dtype)


def call(kernel, outs, args, scratch=(), scalars=0, far=0, flops=1 << 32, vmem=28 << 20):
    specs = [pl.BlockSpec(memory_space=pltpu.SMEM)] * scalars
    specs += [pl.BlockSpec(memory_space=pltpu.VMEM)] * (len(args) - scalars - far)
    specs += [pl.BlockSpec(memory_space=pl.ANY)] * far
    return pl.pallas_call(
        kernel,
        out_shape=outs,
        in_specs=specs,
        out_specs=[pl.BlockSpec(memory_space=pltpu.VMEM)] * len(outs),
        scratch_shapes=scratch,
        compiler_params=pltpu.CompilerParams(vmem_limit_bytes=vmem),
        cost_estimate=pl.CostEstimate(flops=flops, bytes_accessed=1 << 20, transcendentals=0),
    )(*args)


def count_of(axes):
    n = 1
    for a in axes:
        n *= lax.axis_size(a)
    return n


def from_everyone(x, axes):
    spread = jnp.broadcast_to(x[None], (count_of(axes), *x.shape))
    return lax.all_to_all(spread, axes, 0, 0, tiled=True)


def swap_core(x):
    return lax.ppermute(x, "core", [(0, 1), (1, 0)])


def local(node_feats, cotangent, wigner, radial, edge_src, edge_dst, edge_count, params, moment1, moment2):
    nat, coef, chan = node_feats.shape
    rows, _, edges = wigner.shape
    lone = (rows + 2) // 3
    kz, ko = lone * chan, (lone - 1) * chan
    layers, shard = params.shape
    far, near = count_of(FAR), count_of(NEAR)
    core = lax.axis_index("core").astype(jnp.int32).reshape(1)
    odd = lax.axis_index("x") % 2 == 1
    part = (shard + LANES // 2) // LANES
    spare = part * LANES - shard

    half = params.astype(BF16)
    half = jnp.where(odd, jnp.pad(half, ((0, 0), (spare, 0))), jnp.pad(half, ((0, 0), (0, spare))))
    got = from_everyone(half.reshape(layers * part, LANES), FAR).reshape(far * layers * part, LANES)
    mine = from_everyone(got, NEAR)
    other = swap_core(mine)

    x = jnp.transpose(node_feats, (1, 0, 2)).reshape(coef * nat, chan)
    cot = jnp.transpose(cotangent, (1, 0, 2)).reshape(coef * nat, chan)
    live = jnp.arange(edges, dtype=jnp.int32) < edge_count[0]
    dst = jnp.where(live, edge_dst, -1)
    wide = coef * nat
    mats = [sds((rows, edges, wide), BF16), sds((wide, rows * edges), BF16)] * 2
    act = sds((edges, rows * chan), BF16)
    a0, b, bt, d, dt = call(
        functools.partial(prep_kernel, nat),
        [act, *mats],
        (wigner, edge_src.reshape(1, edges), dst.reshape(1, edges), edge_src.reshape(edges, 1), dst.reshape(edges, 1), x, radial[0]),
        vmem=24 << 20,
    )
    block = far * layers * part
    flat = [pltpu.VMEM((layers, (kz * kz + 2 * ko * ko) // LANES, LANES), F32), pltpu.VMEM((2, block, LANES), F32)]
    weights = [pltpu.VMEM((kz, kz), BF16), pltpu.VMEM((ko, ko), BF16), pltpu.VMEM((ko, ko), BF16)]
    space = pltpu.VMEM((edges, rows * chan), BF16)
    held = [pltpu.VMEM(m.shape, m.dtype) for m in mats]
    keep, send = call(
        functools.partial(main_kernel, nat),
        [sds((near, block, LANES), BF16)] * 2,
        (core, mine, other, a0, x, cot, radial[1], b, bt, d, dt),
        [*flat, *weights, space, pltpu.VMEM((rows * edges, chan), BF16), space, *held, pltpu.SemaphoreType.DMA((len(held),))],
        scalars=1,
        far=len(held),
        vmem=44 << 20,
    )
    pair = (keep.astype(F32) + swap_core(send).astype(F32)).astype(BF16)
    arrived = lax.all_to_all(pair, NEAR, 0, 0, tiled=True)
    near_sum = arrived.astype(F32).sum(axis=0).astype(BF16).reshape(far, layers * part, LANES)
    grad = lax.all_to_all(near_sum, FAR, 0, 0, tiled=True).astype(F32).sum(axis=0).reshape(layers, part * LANES)
    grad = jnp.where(odd, grad[:, spare:], grad[:, :shard])

    new_moment1 = 0.9 * moment1 + 0.1 * grad
    new_moment2 = 0.95 * moment2 + 0.05 * grad * grad
    m_hat = new_moment1 / (1.0 - 0.9**60)
    v_hat = new_moment2 / (1.0 - 0.95**60)
    new_params = params - 0.01 * (m_hat / (jnp.sqrt(v_hat) + 1e-08) + 0.1 * params)
    return (new_params, new_moment1, new_moment2)


def solution(mesh):
    fine = Mesh(mesh.devices.reshape(SIZES), AXES)
    flat = P(None, AXES)
    return jax.shard_map(
        local,
        mesh=fine,
        in_specs=(
            P(AXES, None, None),
            P(AXES, None, None),
            P(None, None, AXES),
            P(None, AXES, None),
            P(AXES),
            P(AXES),
            P(AXES),
            flat,
            flat,
            flat,
        ),
        out_specs=(flat, flat, flat),
        check_vma=False,
    )
```
